8 devices in a mesh: batch: 1 (over z), cols: 2 (over y), rows: 4 (over x, core).
Axes of the slice: x: 2, y: 2, z: 1, core: 2. Of those that a mesh axis runs over, the one named last changes fastest.
Arguments:
- frames: bfloat16 [12, 2, 128, 64, 64], P(None, 'batch', 'rows', 'cols')
- w_x: bfloat16 [3, 3, 64, 256], replicated
- w_h: bfloat16 [3, 3, 64, 256], replicated
- gate_bias: float32 [256], replicated
- h_init: bfloat16 [2, 128, 64, 64], P('batch', 'rows', 'cols')
- c_init: float32 [2, 128, 64, 64], P('batch', 'rows', 'cols')
Outputs:
- output 1: bfloat16 [12, 2, 128, 64, 64], P(None, 'batch', 'rows', 'cols')
- output 2: float32 [2, 128, 64, 64], P('batch', 'rows', 'cols')
All inputs are finite; a program needn't handle non-finite values.
Results may differ from the reference program's by a relative error of at most 0.00176749.
Values are sent between devices in bfloat16 or wider.
A program may use at most 1 GiB of HBM per device.

```python
import jax
import jax.numpy as jnp
from jax import lax

STEPS = 12
SAMPLES = 2
GRID_HEIGHT = 128
GRID_WIDTH = 64
IN_CHANNELS = 64
HIDDEN = 64
BAND_ROWS = 8


def setup_inputs(seed: int = 0, part: int = 0) -> dict:
    root_key = jax.random.key(seed)
    shared_key, local_root = jax.random.split(root_key)
    local_key = jax.random.fold_in(local_root, part)
    key_wx, key_wh, key_bias = jax.random.split(shared_key, 3)
    key_frames, key_hidden, key_cell = jax.random.split(local_key, 3)
    gate_width = 4 * HIDDEN
    frames = jax.random.normal(key_frames, (STEPS, SAMPLES, GRID_HEIGHT, GRID_WIDTH, IN_CHANNELS), jnp.float32)
    w_x = jax.random.normal(key_wx, (3, 3, IN_CHANNELS, gate_width), jnp.float32) * (0.8 * (9 * IN_CHANNELS) ** -0.5)
    w_h = jax.random.normal(key_wh, (3, 3, HIDDEN, gate_width), jnp.float32) * (1.5 * (9 * HIDDEN) ** -0.5)
    forget_shift = jnp.concatenate([jnp.zeros((HIDDEN,), jnp.float32), jnp.ones((HIDDEN,), jnp.float32), jnp.zeros((2 * HIDDEN,), jnp.float32)])
    gate_bias = 0.5 * jax.random.normal(key_bias, (gate_width,), jnp.float32) + forget_shift
    h_init = 0.5 * jax.random.normal(key_hidden, (SAMPLES, GRID_HEIGHT, GRID_WIDTH, HIDDEN), jnp.float32)
    c_init = jax.random.normal(key_cell, (SAMPLES, GRID_HEIGHT, GRID_WIDTH, HIDDEN), jnp.float32)
    return {"frames": frames.astype(jnp.bfloat16), "w_x": w_x.astype(jnp.bfloat16), "w_h": w_h.astype(jnp.bfloat16), "gate_bias": gate_bias, "h_init": h_init.astype(jnp.bfloat16), "c_init": c_init}


def conv_taps(padded, weights, out_rows, out_cols):
    tap_list = [padded[:, row_off:row_off + out_rows, col_off:col_off + out_cols, :] for row_off in range(3) for col_off in range(3)]
    patches = jnp.concatenate(tap_list, axis=-1)
    flat_patches = patches.reshape(-1, patches.shape[-1])
    flat_weights = weights.reshape(-1, weights.shape[-1])
    product = jnp.dot(flat_patches, flat_weights, preferred_element_type=jnp.float32)
    return product.reshape(padded.shape[0], out_rows, out_cols, -1)


def lstm_cell(gate_sum, cell_prev):
    hidden_width = cell_prev.shape[-1]
    in_gate = jax.nn.sigmoid(gate_sum[..., :hidden_width])
    forget_gate = jax.nn.sigmoid(gate_sum[..., hidden_width:2 * hidden_width])
    out_gate = jax.nn.sigmoid(gate_sum[..., 2 * hidden_width:3 * hidden_width])
    cand_gate = jnp.tanh(gate_sum[..., 3 * hidden_width:])
    cell_next = forget_gate * cell_prev + in_gate * cand_gate
    hidden_next = (out_gate * jnp.tanh(cell_next)).astype(jnp.bfloat16)
    return hidden_next, cell_next


def reference(frames, w_x, w_h, gate_bias, h_init, c_init):
    num_bands = GRID_HEIGHT // BAND_ROWS
    pad_cfg = ((0, 0), (1, 1), (1, 1), (0, 0))

    def step_fn(state_pair, frame_t):
        hidden, cell_state = state_pair
        frame_pad = jnp.pad(frame_t, pad_cfg)
        hidden_pad = jnp.pad(hidden, pad_cfg)

        def band_update(band_index):
            row_start = band_index * BAND_ROWS
            frame_band = lax.dynamic_slice_in_dim(frame_pad, row_start, BAND_ROWS + 2, axis=1)
            hidden_band = lax.dynamic_slice_in_dim(hidden_pad, row_start, BAND_ROWS + 2, axis=1)
            cell_band = lax.dynamic_slice_in_dim(cell_state, row_start, BAND_ROWS, axis=1)
            gate_sum = conv_taps(frame_band, w_x, BAND_ROWS, GRID_WIDTH) + conv_taps(hidden_band, w_h, BAND_ROWS, GRID_WIDTH) + gate_bias
            return lstm_cell(gate_sum, cell_band)

        band_hidden, band_cell = lax.map(band_update, jnp.arange(num_bands))
        hidden_next = jnp.moveaxis(band_hidden, 0, 1).reshape(SAMPLES, GRID_HEIGHT, GRID_WIDTH, HIDDEN)
        cell_next = jnp.moveaxis(band_cell, 0, 1).reshape(SAMPLES, GRID_HEIGHT, GRID_WIDTH, HIDDEN)
        return (hidden_next, cell_next), hidden_next

    final_pair, all_hidden = lax.scan(step_fn, (h_init, c_init), frames)
    return all_hidden, final_pair[1]
```

```python
import functools

import jax
import jax.numpy as jnp
from jax import lax
from jax.experimental import pallas as pl
from jax.experimental.pallas import tpu as pltpu
from jax.sharding import PartitionSpec as P

MESH = pl.DeviceIdType.MESH
F32, BF16 = jnp.float32, jnp.bfloat16

DEPTH = 3
STEPS = 12
BLOCKS = STEPS // DEPTH
PAIRS = 16
OWN = 64
EDGE = 2
HP = -(-DEPTH // 2)
ROWS_ALL = PAIRS + 2 * EDGE
SUBL = 88
FROM_UP, FROM_DOWN, FROM_SIDE, FROM_DUP, FROM_DDOWN = range(5)
MIRROR = {FROM_UP: FROM_DOWN, FROM_DOWN: FROM_UP, FROM_SIDE: FROM_SIDE, FROM_DUP: FROM_DDOWN, FROM_DDOWN: FROM_DUP}


def region(j):
    halo = DEPTH - 1 - j
    extra = -(-halo // 2)
    return EDGE - extra, PAIRS + 2 * extra, 72 if halo else OWN


def kernel(frames, wx_in, wh_in, bias_in, h_in, c_in, h_out, c_out,
           fbuf, xs, hs, cs, xg, lhs, gts, wx, wh, bias, obuf,
           sx_row, sx_col, sx_cor, sh_row, sh_col, sh_cor, sc_row, sc_col, sc_cor,
           rx_row, rx_col, rx_cor, rh_row, rh_col, rh_cor, rc_row, rc_col, rc_cor,
           fsem, osem, ssem, rsem):
    row, col, grp = lax.axis_index("rows"), lax.axis_index("cols"), lax.axis_index("batch")
    n_rows = 4
    side = 1 - col
    has_up, has_down = row > 0, row < n_rows - 1
    peers = {
        FROM_UP: (has_up, row - 1, col),
        FROM_DOWN: (has_down, row + 1, col),
        FROM_SIDE: (None, row, side),
        FROM_DUP: (has_up, row - 1, side),
        FROM_DDOWN: (has_down, row + 1, side),
    }

    def guarded(cond, fn):
        if cond is None:
            fn()
        else:
            pl.when(cond)(fn)

    lane = lax.broadcasted_iota(jnp.int32, (72, 128), 1)
    subl = lax.broadcasted_iota(jnp.int32, (8, 128), 0)
    col_mask = jnp.where((subl + 2 * (1 - col) >= 2) & (subl < 6 + 2 * col), 1.0, 0.0).astype(F32)
    up_mask = jnp.where(has_up, 1.0, 0.0).astype(F32)
    down_mask = jnp.where(has_down, 1.0, 0.0).astype(F32)

    def frame_copy(t, slot):
        return pltpu.make_async_copy(frames.at[t], fbuf.at[slot], fsem.at[slot])

    for j in range(DEPTH):
        frame_copy(j, j).start()

    barrier = pltpu.get_barrier_semaphore()
    for cond, r, c in peers.values():
        guarded(cond, lambda r=r, c=c: pl.semaphore_signal(barrier, inc=1, device_id=(grp, c, r), device_id_type=MESH))

    def ingest(load, dst):
        def body(i, _):
            for u in range(4):
                q = i * 4 + u
                for s in range(2):
                    both = jnp.concatenate([load(s, 2 * q), load(s, 2 * q + 1)], axis=1).astype(F32)
                    dst[q, pl.ds(s, 32, stride=2), :] = both
            return 0
        lax.fori_loop(0, PAIRS // 4, body, 0)

    def wrap_first(ref, q):
        ref[q, 80:88, :] = ref[q, 8:16, :]

    hs[...] = jnp.zeros_like(hs)
    cs[...] = jnp.zeros_like(cs)
    xs[...] = jnp.zeros_like(xs)

    ingest(lambda s, r: h_in[s, r], hs.at[pl.ds(EDGE, PAIRS), pl.ds(8, OWN)])
    ingest(lambda s, r: c_in[s, r], cs.at[pl.ds(1, PAIRS), pl.ds(0, OWN)])
    for q in range(PAIRS):
        wrap_first(hs, EDGE + q)

    strip_at = pl.multiple_of(8 + 56 * (1 - col), 8)
    cstrip_at = pl.multiple_of(56 * (1 - col), 8)

    def pack_bf16(src, s_row, s_col, s_cor):
        for p in range(HP):
            s_row[0, p] = src[EDGE + p, 8:72, :].astype(BF16)
            s_row[1, p] = src[EDGE + PAIRS - HP + p, 8:72, :].astype(BF16)
        two = []
        for i in range(PAIRS // 2):
            two.append(jnp.concatenate([src[EDGE + 2 * i, pl.ds(strip_at, 8), :],
                                        src[EDGE + 2 * i + 1, pl.ds(strip_at, 8), :]], axis=0).astype(BF16))
            s_col[i] = two[-1]
        s_cor[0] = two[0]
        s_cor[1] = two[-1]

    def unpack_side(dst, q, strip):
        strip = strip * col_mask
        dst[q, 72:80, :] = strip
        dst[q, 0:8, :] = strip

    def unpack_bf16(dst, get_row, get_col, get_cor):
        for i in range(PAIRS // 2):
            both = get_col(i).astype(F32)
            unpack_side(dst, EDGE + 2 * i, both[0:8])
            unpack_side(dst, EDGE + 2 * i + 1, both[8:16])

        def rows(which, first):
            for p in range(HP):
                strip = get_row(which, p).astype(F32)
                dst[first + p, 8:72, :] = strip
                dst[first + p, 80:88, :] = strip[0:8]
            both = get_cor(which).astype(F32)
            for p in range(HP):
                at = 2 - HP + p if which == 0 else p
                unpack_side(dst, first + p, both[8 * at:8 * at + 8])

        pl.when(has_up)(lambda: rows(0, EDGE - HP))
        pl.when(has_down)(lambda: rows(1, EDGE + PAIRS))

    def copies(b, kind, sends, recvs):
        s_row, s_col, s_cor = sends
        r_row, r_col, r_cor = recvs
        out = []
        for d, (cond, r, c) in peers.items():
            m = MIRROR[d]
            if d in (FROM_UP, FROM_DOWN):
                src, dst = s_row.at[d], r_row.at[m]
            elif d == FROM_SIDE:
                src, dst = s_col, r_col
            else:
                src, dst = s_cor.at[d - FROM_DUP], r_cor.at[m - FROM_DUP]
            out.append((cond, pltpu.make_async_remote_copy(
                src_ref=src, dst_ref=dst, send_sem=ssem.at[b, kind, d], recv_sem=rsem.at[b, kind, m],
                device_id=(grp, c, r), device_id_type=MESH)))
        return out

    def waits(b, kind, sends, recvs):
        s_row, s_col, s_cor = sends
        r_row, r_col, r_cor = recvs
        out = []
        for d, (cond, r, c) in peers.items():
            if d in (FROM_UP, FROM_DOWN):
                src, dst = s_row.at[d], r_row.at[d]
            elif d == FROM_SIDE:
                src, dst = s_col, r_col
            else:
                src, dst = s_cor.at[d - FROM_DUP], r_cor.at[d - FROM_DUP]
            out.append((cond, pltpu.make_async_remote_copy(
                src_ref=src, dst_ref=dst, send_sem=ssem.at[b, kind, d], recv_sem=rsem.at[b, kind, d],
                device_id=(grp, c, r), device_id_type=MESH)))
        return out

    def bufs(b, kind):
        if kind == 0:
            return ((sx_row.at[b], sx_col.at[b], sx_cor.at[b]), (rx_row.at[b], rx_col.at[b], rx_cor.at[b]))
        if kind == 1:
            return ((sh_row.at[b], sh_col.at[b], sh_cor.at[b]), (rh_row.at[b], rh_col.at[b], rh_cor.at[b]))
        return ((sc_row.at[b], sc_col.at[b], sc_cor.at[b]), (rc_row.at[b], rc_col.at[b], rc_cor.at[b]))

    def send(b, kind):
        for cond, cp in copies(b, kind, *bufs(b, kind)):
            guarded(cond, lambda cp=cp: cp.start())

    def receive(b, kind):
        for cond, cp in waits(b, kind, *bufs(b, kind)):
            guarded(cond, lambda cp=cp: cp.wait_recv())

    def send_state(b):
        pack_bf16(hs, sh_row.at[b], sh_col.at[b], sh_cor.at[b])
        if DEPTH > 1:
            sc_row[b, 0] = cs[1, 0:OWN, :]
            sc_row[b, 1] = cs[PAIRS, 0:OWN, :]
            for q in range(PAIRS):
                sc_col[b, q] = cs[1 + q, pl.ds(cstrip_at, 8), :]
            sc_cor[b, 0] = cs[1, pl.ds(cstrip_at, 8), :]
            sc_cor[b, 1] = cs[PAIRS, pl.ds(cstrip_at, 8), :]
        send(b, 1)
        if DEPTH > 1:
            send(b, 2)

    def receive_state(b):
        receive(b, 1)
        unpack_bf16(hs, lambda w, p: rh_row[b, w, p], lambda i: rh_col[b, i], lambda w: rh_cor[b, w])
        if DEPTH > 1:
            receive(b, 2)
            for q in range(PAIRS):
                cs[1 + q, 64:72, :] = rc_col[b, q]

            def rows(which, at):
                cs[at, 0:OWN, :] = rc_row[b, which]
                cs[at, 64:72, :] = rc_cor[b, which]

            pl.when(has_up)(lambda: rows(0, 0))
            pl.when(has_down)(lambda: rows(1, 1 + PAIRS))

    def send_frames(b):
        for j in range(DEPTH):
            frame_copy(0, j).wait()
            ingest(lambda s, r: fbuf[j, s, r], xs.at[j, pl.ds(EDGE, PAIRS), pl.ds(8, OWN)])
            for q in range(PAIRS):
                wrap_first(xs.at[j], EDGE + q)
            pack_bf16(xs.at[j], sx_row.at[b, :, j], sx_col.at[b, j], sx_cor.at[b, :, j])
        send(b, 0)

        @pl.when(b + 1 < BLOCKS)
        def _():
            for j in range(DEPTH):
                frame_copy((b + 1) * DEPTH + j, j).start()

    def build(src, j):
        first, count, width = region(j)
        low = (lane < 64)[0:width]
        for q in range(0, count, 2):
            for dx in range(3):
                at = pl.ds(6 + 2 * dx, width)
                r = [src[first + q + i, at, :] for i in range(-1, 3)]
                own = jnp.concatenate([r[1], r[2]], axis=0).astype(BF16)
                near = jnp.concatenate([jnp.where(low, r[2], r[0]), jnp.where(low, r[3], r[1])], axis=0).astype(BF16)
                lhs[q * width:(q + 2) * width, dx * 256:dx * 256 + 128] = own
                lhs[q * width:(q + 2) * width, dx * 256 + 128:dx * 256 + 256] = near

    def chunks(j):
        first, count, width = region(j)
        step = 6 if count == 18 else 8
        return [(g, step) for g in range(0, count, step)]

    def conv_x(b):
        receive(b, 0)
        for j in range(DEPTH):
            unpack_bf16(xs.at[j], lambda w, p: rx_row[b, w, j, p], lambda i: rx_col[b, j, i], lambda w: rx_cor[b, w, j])
        for j in range(DEPTH):
            first, count, width = region(j)
            build(xs.at[j], j)
            for g, n in chunks(j):
                rows = pl.ds(g * width, n * width)
                xg[j, rows, :] = jnp.dot(lhs[rows, :], wx[...], preferred_element_type=F32) + bias[...]

    def step(j):
        first, count, width = region(j)
        build(hs, j)
        for g, n in chunks(j):
            rows = pl.ds(g * width, n * width)
            gts[rows, :] = jnp.dot(lhs[rows, :], wh[...], preferred_element_type=F32) + xg[j, rows, :]
            for q in range(g, g + n):
                rows_q = pl.ds(q * width, width)
                gi, gf, go, gg = (gts[rows_q, 128 * i:128 * i + 128] for i in range(4))
                at = first + q
                c_old = cs[at - 1, 0:width, :]
                ti, tf, to = jnp.tanh(0.5 * gi), jnp.tanh(0.5 * gf), jnp.tanh(0.5 * go)
                c_new = 0.5 * ((tf + 1.0) * c_old + (ti + 1.0) * jnp.tanh(gg))
                cs[at - 1, 0:width, :] = c_new
                h_new = 0.5 * (to + 1.0) * jnp.tanh(c_new)
                if at < EDGE:
                    h_new = h_new * up_mask
                if at >= EDGE + PAIRS:
                    h_new = h_new * down_mask
                hs[at, 8:72, :] = h_new[0:OWN]
                hs[at, 80:88, :] = h_new[0:8]
                if width == 72:
                    unpack_side(hs, at, h_new[64:72])

    def out_copy(t, j):
        return pltpu.make_async_copy(obuf.at[j], h_out.at[t], osem.at[j])

    def emit(b, j):
        @pl.when(b > 0)
        def _():
            out_copy(0, j).wait()

        def body(i, _):
            for u in range(4):
                q = i * 4 + u
                for s in range(2):
                    both = hs[EDGE + q, pl.ds(8 + s, 32, stride=2), :].astype(BF16)
                    obuf[j, s, 2 * q] = both[:, 0:64]
                    obuf[j, s, 2 * q + 1] = both[:, 64:128]
            return 0

        lax.fori_loop(0, PAIRS // 4, body, 0)
        out_copy(b * DEPTH + j, j).start()

    def weights(src, dst):
        zero = jnp.zeros((64, 64), BF16)
        for dx in range(3):
            for k, q in enumerate((0, 1, 2, -1)):
                for g in range(4):
                    parts = []
                    for p in range(2):
                        dy = q - p + 1
                        parts.append(src[dy, dx, :, 64 * g:64 * g + 64] if 0 <= dy <= 2 else zero)
                    dst[dx * 256 + k * 64:dx * 256 + k * 64 + 64, 128 * g:128 * g + 128] = jnp.concatenate(parts, axis=1)

    count = 3 + 2 * (has_up & has_down).astype(jnp.int32)
    pl.semaphore_wait(barrier, count)
    send_state(0)
    send_frames(0)
    weights(wx_in, wx)
    weights(wh_in, wh)
    for g in range(4):
        piece = bias_in[:, 64 * g:64 * g + 64]
        bias[:, 128 * g:128 * g + 128] = jnp.concatenate([piece, piece], axis=1)
    conv_x(0)

    def block(b, _):
        @pl.when(b + 1 < BLOCKS)
        def _():
            send_frames(b + 1)

        receive_state(b)
        for j in range(DEPTH):
            step(j)
            emit(b, j)

        @pl.when(b + 1 < BLOCKS)
        def _():
            send_state(b + 1)
            conv_x(b + 1)

        return 0

    lax.fori_loop(0, BLOCKS, block, 0)

    def final(i, _):
        for u in range(4):
            q = i * 4 + u
            for s in range(2):
                both = cs[1 + q, pl.ds(s, 32, stride=2), :]
                c_out[s, 2 * q] = both[:, 0:64]
                c_out[s, 2 * q + 1] = both[:, 64:128]
        return 0

    lax.fori_loop(0, PAIRS // 4, final, 0)
    for j in range(DEPTH):
        out_copy(0, j).wait()

    def drain(b, _):
        for kind in range(3 if DEPTH > 1 else 2):
            for cond, cp in copies(b, kind, *bufs(b, kind)):
                guarded(cond, lambda cp=cp: cp.wait_send())
        return 0

    lax.fori_loop(0, BLOCKS, drain, 0)


def solution(mesh):
    frame_spec = P(None, "batch", "rows", "cols", None)
    state_spec = P("batch", "rows", "cols", None)

    def local_run(frames, w_x, w_h, gate_bias, h_init, c_init):
        vmem = pl.BlockSpec(memory_space=pltpu.VMEM)
        hbm = pl.BlockSpec(memory_space=pl.ANY)
        most = max(region(j)[1] * region(j)[2] for j in range(DEPTH))
        strips = [
            [(BLOCKS, 2, DEPTH, HP, OWN, 128), (BLOCKS, DEPTH, 8, 16, 128), (BLOCKS, 2, DEPTH, 16, 128)],
            [(BLOCKS, 2, HP, OWN, 128), (BLOCKS, 8, 16, 128), (BLOCKS, 2, 16, 128)],
            [(BLOCKS, 2, OWN, 128), (BLOCKS, PAIRS, 8, 128), (BLOCKS, 2, 8, 128)],
        ]
        strip_bufs = [pltpu.VMEM(s, BF16 if k < 2 else F32) for k in range(3) for s in strips[k]]
        return pl.pallas_call(
            kernel,
            out_shape=(jax.ShapeDtypeStruct(frames.shape, BF16), jax.ShapeDtypeStruct(c_init.shape, F32)),
            in_specs=[hbm, vmem, vmem, vmem, vmem, vmem],
            out_specs=(hbm, vmem),
            scratch_shapes=[
                pltpu.VMEM((DEPTH,) + h_init.shape, BF16),
                pltpu.VMEM((DEPTH, ROWS_ALL, SUBL, 128), F32),
                pltpu.VMEM((ROWS_ALL, SUBL, 128), F32),
                pltpu.VMEM((PAIRS + 2, 72, 128), F32),
                pltpu.VMEM((DEPTH, most, 512), F32),
                pltpu.VMEM((most, 768), BF16),
                pltpu.VMEM((most, 512), F32),
                pltpu.VMEM((768, 512), BF16),
                pltpu.VMEM((768, 512), BF16),
                pltpu.VMEM((1, 512), F32),
                pltpu.VMEM((DEPTH,) + h_init.shape, BF16),
                *strip_bufs, *strip_bufs,
                pltpu.SemaphoreType.DMA((DEPTH,)),
                pltpu.SemaphoreType.DMA((DEPTH,)),
                pltpu.SemaphoreType.DMA((BLOCKS, 3, 5)),
                pltpu.SemaphoreType.DMA((BLOCKS, 3, 5)),
            ],
            compiler_params=pltpu.CompilerParams(collective_id=0, has_side_effects=True, vmem_limit_bytes=60 * 2**20),
        )(frames, w_x, w_h, gate_bias.reshape(1, 256), h_init, c_init)

    return jax.shard_map(local_run, mesh=mesh, in_specs=(frame_spec, P(), P(), P(), state_spec, state_spec),
                         out_specs=(frame_spec, state_spec), check_vma=False)
```

```python
import functools

import jax
import jax.numpy as jnp
from jax import lax
from jax.experimental import pallas as pl
from jax.experimental.pallas import tpu as pltpu
from jax.sharding import PartitionSpec as P

MESH = pl.DeviceIdType.MESH
F32, BF16 = jnp.float32, jnp.bfloat16

DEPTH = 3
STEPS = 12
BLOCKS = STEPS // DEPTH
PAIRS = 16
OWN = 64
EDGE = 2
HP = -(-DEPTH // 2)
ROWS_ALL = PAIRS + 2 * EDGE
SUBL = 88
FROM_UP, FROM_DOWN, FROM_SIDE, FROM_DUP, FROM_DDOWN = range(5)
MIRROR = {FROM_UP: FROM_DOWN, FROM_DOWN: FROM_UP, FROM_SIDE: FROM_SIDE, FROM_DUP: FROM_DDOWN, FROM_DDOWN: FROM_DUP}


def region(j):
    halo = DEPTH - 1 - j
    extra = -(-halo // 2)
    return EDGE - extra, PAIRS + 2 * extra, 72 if halo else OWN


def kernel(frames, wx_in, wh_in, bias_in, h_in, c_in, h_out, c_out,
           fbuf, xs, hs, cs, xg, lhs, gts, wx, wh, bias, obuf,
           sx_row, sx_col, sx_cor, sh_row, sh_col, sh_cor, sc_row, sc_col, sc_cor,
           rx_row, rx_col, rx_cor, rh_row, rh_col, rh_cor, rc_row, rc_col, rc_cor,
           fsem, osem, ssem, rsem):
    row, col, grp = lax.axis_index("rows"), lax.axis_index("cols"), lax.axis_index("batch")
    n_rows = 4
    side = 1 - col
    has_up, has_down = row > 0, row < n_rows - 1
    peers = {
        FROM_UP: (has_up, row - 1, col),
        FROM_DOWN: (has_down, row + 1, col),
        FROM_SIDE: (None, row, side),
        FROM_DUP: (has_up, row - 1, side),
        FROM_DDOWN: (has_down, row + 1, side),
    }

    def guarded(cond, fn):
        if cond is None:
            fn()
        else:
            pl.when(cond)(fn)

    lane = lax.broadcasted_iota(jnp.int32, (72, 128), 1)
    subl = lax.broadcasted_iota(jnp.int32, (8, 128), 0)
    col_mask = jnp.where((subl + 2 * (1 - col) >= 2) & (subl < 6 + 2 * col), 1.0, 0.0).astype(F32)
    up_mask = jnp.where(has_up, 1.0, 0.0).astype(F32)
    down_mask = jnp.where(has_down, 1.0, 0.0).astype(F32)

    def frame_copy(t, slot):
        return pltpu.make_async_copy(frames.at[t], fbuf.at[slot], fsem.at[slot])

    for j in range(DEPTH):
        frame_copy(j, j).start()

    barrier = pltpu.get_barrier_semaphore()
    for cond, r, c in peers.values():
        guarded(cond, lambda r=r, c=c: pl.semaphore_signal(barrier, inc=1, device_id=(grp, c, r), device_id_type=MESH))

    def ingest(load, dst):
        def body(i, _):
            for u in range(4):
                q = i * 4 + u
                for s in range(2):
                    both = jnp.concatenate([load(s, 2 * q), load(s, 2 * q + 1)], axis=1).astype(F32)
                    dst[q, pl.ds(s, 32, stride=2), :] = both
            return 0
        lax.fori_loop(0, PAIRS // 4, body, 0)

    def wrap_first(ref, q):
        ref[q, 80:88, :] = ref[q, 8:16, :]

    hs[...] = jnp.zeros_like(hs)
    cs[...] = jnp.zeros_like(cs)
    xs[...] = jnp.zeros_like(xs)

    ingest(lambda s, r: h_in[s, r], hs.at[pl.ds(EDGE, PAIRS), pl.ds(8, OWN)])
    ingest(lambda s, r: c_in[s, r], cs.at[pl.ds(1, PAIRS), pl.ds(0, OWN)])
    for q in range(PAIRS):
        wrap_first(hs, EDGE + q)

    strip_at = pl.multiple_of(8 + 56 * (1 - col), 8)
    cstrip_at = pl.multiple_of(56 * (1 - col), 8)
    cstrip_from = pl.multiple_of(60 * (1 - col), 4)
    cstrip_to = pl.multiple_of(64 + 4 * col, 4)

    def pack_bf16(src, s_row, s_col, s_cor):
        for p in range(HP):
            s_row[0, p] = src[EDGE + p, 8:72, :].astype(BF16)
            s_row[1, p] = src[EDGE + PAIRS - HP + p, 8:72, :].astype(BF16)
        two = []
        for i in range(PAIRS // 2):
            two.append(jnp.concatenate([src[EDGE + 2 * i, pl.ds(strip_at, 8), :],
                                        src[EDGE + 2 * i + 1, pl.ds(strip_at, 8), :]], axis=0).astype(BF16))
            s_col[i] = two[-1]
        s_cor[0] = two[0]
        s_cor[1] = two[-1]

    def unpack_side(dst, q, strip):
        strip = strip * col_mask
        dst[q, 72:80, :] = strip
        dst[q, 0:8, :] = strip

    def unpack_bf16(dst, get_row, get_col, get_cor):
        for i in range(PAIRS // 2):
            both = get_col(i).astype(F32)
            unpack_side(dst, EDGE + 2 * i, both[0:8])
            unpack_side(dst, EDGE + 2 * i + 1, both[8:16])

        def rows(which, first):
            for p in range(HP):
                strip = get_row(which, p).astype(F32)
                dst[first + p, 8:72, :] = strip
                dst[first + p, 80:88, :] = strip[0:8]
            both = get_cor(which).astype(F32)
            for p in range(HP):
                at = 2 - HP + p if which == 0 else p
                unpack_side(dst, first + p, both[8 * at:8 * at + 8])

        pl.when(has_up)(lambda: rows(0, EDGE - HP))
        pl.when(has_down)(lambda: rows(1, EDGE + PAIRS))

    def copies(b, kind, sends, recvs):
        s_row, s_col, s_cor = sends
        r_row, r_col, r_cor = recvs
        out = []
        for d, (cond, r, c) in peers.items():
            m = MIRROR[d]
            if d in (FROM_UP, FROM_DOWN):
                src, dst = s_row.at[d], r_row.at[m]
            elif d == FROM_SIDE:
                src, dst = s_col, r_col
            else:
                src, dst = s_cor.at[d - FROM_DUP], r_cor.at[m - FROM_DUP]
            out.append((cond, pltpu.make_async_remote_copy(
                src_ref=src, dst_ref=dst, send_sem=ssem.at[b, kind, d], recv_sem=rsem.at[b, kind, m],
                device_id=(grp, c, r), device_id_type=MESH)))
        return out

    def waits(b, kind, sends, recvs):
        s_row, s_col, s_cor = sends
        r_row, r_col, r_cor = recvs
        out = []
        for d, (cond, r, c) in peers.items():
            if d in (FROM_UP, FROM_DOWN):
                src, dst = s_row.at[d], r_row.at[d]
            elif d == FROM_SIDE:
                src, dst = s_col, r_col
            else:
                src, dst = s_cor.at[d - FROM_DUP], r_cor.at[d - FROM_DUP]
            out.append((cond, pltpu.make_async_remote_copy(
                src_ref=src, dst_ref=dst, send_sem=ssem.at[b, kind, d], recv_sem=rsem.at[b, kind, d],
                device_id=(grp, c, r), device_id_type=MESH)))
        return out

    def bufs(b, kind):
        if kind < DEPTH:
            return ((sx_row.at[b, kind], sx_col.at[b, kind], sx_cor.at[b, kind]),
                    (rx_row.at[b, kind], rx_col.at[b, kind], rx_cor.at[b, kind]))
        if kind == DEPTH:
            return ((sh_row.at[b], sh_col.at[b], sh_cor.at[b]), (rh_row.at[b], rh_col.at[b], rh_cor.at[b]))
        return ((sc_row.at[b], sc_col.at[b], sc_cor.at[b]), (rc_row.at[b], rc_col.at[b], rc_cor.at[b]))

    def send(b, kind):
        for cond, cp in copies(b, kind, *bufs(b, kind)):
            guarded(cond, lambda cp=cp: cp.start())

    def receive(b, kind):
        for cond, cp in waits(b, kind, *bufs(b, kind)):
            guarded(cond, lambda cp=cp: cp.wait_recv())

    def send_state(b):
        pack_bf16(hs, sh_row.at[b], sh_col.at[b], sh_cor.at[b])
        if DEPTH > 1:
            sc_row[b, 0] = cs[1, 0:OWN, :]
            sc_row[b, 1] = cs[PAIRS, 0:OWN, :]
            for q in range(PAIRS):
                sc_col[b, q // 2, 4 * (q % 2):4 * (q % 2) + 4] = cs[1 + q, pl.ds(cstrip_from, 4), :]
            sc_cor[b, 0] = cs[1, pl.ds(cstrip_at, 8), :]
            sc_cor[b, 1] = cs[PAIRS, pl.ds(cstrip_at, 8), :]
        send(b, DEPTH)
        if DEPTH > 1:
            send(b, DEPTH + 1)

    def receive_state(b):
        receive(b, DEPTH)
        unpack_bf16(hs, lambda w, p: rh_row[b, w, p], lambda i: rh_col[b, i], lambda w: rh_cor[b, w])
        if DEPTH > 1:
            receive(b, DEPTH + 1)
            for q in range(PAIRS):
                cs[1 + q, pl.ds(cstrip_to, 4), :] = rc_col[b, q // 2, 4 * (q % 2):4 * (q % 2) + 4]

            def rows(which, at):
                cs[at, 0:OWN, :] = rc_row[b, which]
                cs[at, 64:72, :] = rc_cor[b, which]

            pl.when(has_up)(lambda: rows(0, 0))
            pl.when(has_down)(lambda: rows(1, 1 + PAIRS))

    def take_frame(b, j, pairs):
        for q in pairs:
            for s in range(2):
                both = jnp.concatenate([fbuf[j, s, 2 * q], fbuf[j, s, 2 * q + 1]], axis=1).astype(F32)
                xs[j, EDGE + q, pl.ds(8 + s, 32, stride=2), :] = both
            wrap_first(xs.at[j], EDGE + q)

    def pack_frame(b, j):
        pack_bf16(xs.at[j], sx_row.at[b, j], sx_col.at[b, j], sx_cor.at[b, j])

    def tasks(j):
        first, count, width = region(j)
        n = 6 if count == 18 else 8
        return [(j, first + g, n, width, g * width) for g in range(0, count, n)]

    def build(src, slot, task):
        _, first, n, width, _ = task
        low = (lane < 64)[0:width]
        for q in range(0, n, 2):
            for dx in range(3):
                at = pl.ds(6 + 2 * dx, width)
                r = [src[first + q + i, at, :] for i in range(-1, 3)]
                own = jnp.concatenate([r[1], r[2]], axis=0).astype(BF16)
                near = jnp.concatenate([jnp.where(low, r[2], r[0]), jnp.where(low, r[3], r[1])], axis=0).astype(BF16)
                lhs[slot, q * width:(q + 2) * width, dx * 256:dx * 256 + 128] = own
                lhs[slot, q * width:(q + 2) * width, dx * 256 + 128:dx * 256 + 256] = near

    def product(slot, task, w):
        _, _, n, width, _ = task
        return jnp.dot(lhs[slot, 0:n * width, :], w[...], preferred_element_type=F32)

    def conv_x(b, following):
        for j in range(DEPTH):
            receive(b, j)
        for j in range(DEPTH):
            unpack_bf16(xs.at[j], lambda w, p: rx_row[b, j, w, p], lambda i: rx_col[b, j, i], lambda w: rx_cor[b, j, w])

        @pl.when(following < BLOCKS)
        def _():
            for j in range(DEPTH):
                frame_copy(0, j).wait()

        todo = [t for j in range(DEPTH) for t in tasks(j)]
        build(xs.at[0], 0, todo[0])
        for i, task in enumerate(todo):
            if i + 1 < len(todo):
                build(xs.at[todo[i + 1][0]], (i + 1) % 2, todo[i + 1])
            j, _, n, width, at = task
            xg[j, at:at + n * width, :] = product(i % 2, task, wx) + bias[...]
            if i + 1 == len(todo) or todo[i + 1][0] != j:
                take_frame(following, j, range(PAIRS))
                pack_frame(following, j)

        @pl.when(following < BLOCKS)
        def _():
            for j in range(DEPTH):
                send(following, j)

        @pl.when(following + 1 < BLOCKS)
        def _():
            for j in range(DEPTH):
                frame_copy((following + 1) * DEPTH + j, j).start()

    def cells(slot, task):
        j, first, n, width, base = task
        gts[slot, 0:n * width, :] = product(slot, task, wh) + xg[j, base:base + n * width, :]
        for q in range(n):
            rows_q = pl.ds(q * width, width)
            gi, gf, go, gg = (gts[slot, rows_q, 128 * i:128 * i + 128] for i in range(4))
            at = first + q
            c_old = cs[at - 1, 0:width, :]
            ti, tf, to = jnp.tanh(0.5 * gi), jnp.tanh(0.5 * gf), jnp.tanh(0.5 * go)
            c_new = 0.5 * ((tf + 1.0) * c_old + (ti + 1.0) * jnp.tanh(gg))
            cs[at - 1, 0:width, :] = c_new
            h_new = 0.5 * (to + 1.0) * jnp.tanh(c_new)
            if at < EDGE:
                h_new = h_new * up_mask
            if at >= EDGE + PAIRS:
                h_new = h_new * down_mask
            hs[at, 8:72, :] = h_new[0:OWN]
            hs[at, 80:88, :] = h_new[0:8]
            if width == 72:
                unpack_side(hs, at, h_new[64:72])
            if EDGE <= at < EDGE + PAIRS:
                for s in range(2):
                    obuf[j, s, at - EDGE] = hs[at, pl.ds(8 + s, 32, stride=2), :].astype(BF16)

    def out_copy(t, j):
        return pltpu.make_async_copy(obuf.at[j], h_out.at[t], osem.at[j])

    def steps(b):
        @pl.when(b > 0)
        def _():
            for j in range(DEPTH):
                out_copy(0, j).wait()

        todo = [t for j in range(DEPTH) for t in tasks(j)]
        build(hs, 0, todo[0])
        for i, task in enumerate(todo):
            if i + 1 < len(todo):
                build(hs, (i + 1) % 2, todo[i + 1])
            cells(i % 2, task)
            if i + 1 == len(todo) or todo[i + 1][0] != task[0]:
                out_copy(b * DEPTH + task[0], task[0]).start()

    def weights(src, dst):
        zero = jnp.zeros((64, 64), BF16)
        for dx in range(3):
            for k, q in enumerate((0, 1, 2, -1)):
                for g in range(4):
                    parts = []
                    for p in range(2):
                        dy = q - p + 1
                        parts.append(src[dy, dx, :, 64 * g:64 * g + 64] if 0 <= dy <= 2 else zero)
                    dst[dx * 256 + k * 64:dx * 256 + k * 64 + 64, 128 * g:128 * g + 128] = jnp.concatenate(parts, axis=1)

    for j in range(DEPTH):
        frame_copy(0, j).wait()
        ingest(lambda s, r: fbuf[j, s, r], xs.at[j, pl.ds(EDGE, PAIRS), pl.ds(8, OWN)])
        for q in range(PAIRS):
            wrap_first(xs.at[j], EDGE + q)
        pack_frame(0, j)
    for j in range(DEPTH):
        frame_copy(DEPTH + j, j).start()
    count = 3 + 2 * (has_up & has_down).astype(jnp.int32)
    pl.semaphore_wait(barrier, count)
    for j in range(DEPTH):
        send(0, j)
    send_state(0)
    weights(wx_in, wx)
    weights(wh_in, wh)
    for g in range(4):
        piece = bias_in[:, 64 * g:64 * g + 64]
        bias[:, 128 * g:128 * g + 128] = jnp.concatenate([piece, piece], axis=1)
    conv_x(0, 1)

    def block(b, _):
        receive_state(b)
        steps(b)
        send_state(b + 1)
        conv_x(b + 1, b + 2)
        return 0

    lax.fori_loop(0, BLOCKS - 1, block, 0)
    receive_state(BLOCKS - 1)
    steps(BLOCKS - 1)

    for q in range(PAIRS):
        for s in range(2):
            c_out[s, q] = cs[1 + q, pl.ds(s, 32, stride=2), :]
    for j in range(DEPTH):
        out_copy(0, j).wait()

    def drain(b, _):
        for kind in range(DEPTH + 2 if DEPTH > 1 else DEPTH + 1):
            for cond, cp in copies(b, kind, *bufs(b, kind)):
                guarded(cond, lambda cp=cp: cp.wait_send())
        return 0

    lax.fori_loop(0, BLOCKS, drain, 0)


def expand(h_ref, c_ref, h_out, c_out):
    for s in range(2):
        for q in range(PAIRS):
            both = h_ref[0, s, q]
            h_out[0, s, 2 * q] = both[:, 0:64]
            h_out[0, s, 2 * q + 1] = both[:, 64:128]

    @pl.when(pl.program_id(0) == 0)
    def _():
        for s in range(2):
            for q in range(PAIRS):
                both = c_ref[s, q]
                c_out[s, 2 * q] = both[:, 0:64]
                c_out[s, 2 * q + 1] = both[:, 64:128]


def solution(mesh):
    frame_spec = P(None, "batch", "rows", "cols", None)
    state_spec = P("batch", "rows", "cols", None)

    def local_run(frames, w_x, w_h, gate_bias, h_init, c_init):
        vmem = pl.BlockSpec(memory_space=pltpu.VMEM)
        hbm = pl.BlockSpec(memory_space=pl.ANY)
        most = max(region(j)[1] * region(j)[2] for j in range(DEPTH))
        strips = [
            [(BLOCKS, DEPTH, 2, HP, OWN, 128), (BLOCKS, DEPTH, 8, 16, 128), (BLOCKS, DEPTH, 2, 16, 128)],
            [(BLOCKS, 2, HP, OWN, 128), (BLOCKS, 8, 16, 128), (BLOCKS, 2, 16, 128)],
            [(BLOCKS, 2, OWN, 128), (BLOCKS, PAIRS // 2, 8, 128), (BLOCKS, 2, 8, 128)],
        ]
        recv_bufs = [pltpu.VMEM(s, BF16 if k < 2 else F32) for k in range(3) for s in strips[k]]
        strips[0] = [(s[0] + 1,) + s[1:] for s in strips[0]]
        send_bufs = [pltpu.VMEM(s, BF16 if k < 2 else F32) for k in range(3) for s in strips[k]]
        h_pairs, c_pairs = pl.pallas_call(
            kernel,
            out_shape=(jax.ShapeDtypeStruct((STEPS, 2, PAIRS, 32, 128), BF16),
                       jax.ShapeDtypeStruct((2, PAIRS, 32, 128), F32)),
            in_specs=[hbm, vmem, vmem, vmem, vmem, vmem],
            out_specs=(hbm, vmem),
            scratch_shapes=[
                pltpu.VMEM((DEPTH,) + h_init.shape, BF16),
                pltpu.VMEM((DEPTH, ROWS_ALL, SUBL, 128), F32),
                pltpu.VMEM((ROWS_ALL, SUBL, 128), F32),
                pltpu.VMEM((PAIRS + 2, 72, 128), F32),
                pltpu.VMEM((DEPTH, most, 512), F32),
                pltpu.VMEM((2, 512, 768), BF16),
                pltpu.VMEM((2, 512, 512), F32),
                pltpu.VMEM((768, 512), BF16),
                pltpu.VMEM((768, 512), BF16),
                pltpu.VMEM((1, 512), F32),
                pltpu.VMEM((DEPTH, 2, PAIRS, 32, 128), BF16),
                *send_bufs, *recv_bufs,
                pltpu.SemaphoreType.DMA((DEPTH,)),
                pltpu.SemaphoreType.DMA((DEPTH,)),
                pltpu.SemaphoreType.DMA((BLOCKS, DEPTH + 2, 5)),
                pltpu.SemaphoreType.DMA((BLOCKS, DEPTH + 2, 5)),
            ],
            compiler_params=pltpu.CompilerParams(collective_id=0, has_side_effects=True, vmem_limit_bytes=60 * 2**20),
        )(frames, w_x, w_h, gate_bias.reshape(1, 256), h_init, c_init)
        return pl.pallas_call(
            expand,
            grid=(STEPS,),
            out_shape=(jax.ShapeDtypeStruct(frames.shape, BF16), jax.ShapeDtypeStruct(c_init.shape, F32)),
            in_specs=[pl.BlockSpec((1, 2, PAIRS, 32, 128), lambda t: (t, 0, 0, 0, 0)),
                      pl.BlockSpec((2, PAIRS, 32, 128), lambda t: (0, 0, 0, 0))],
            out_specs=(pl.BlockSpec((1,) + frames.shape[1:], lambda t: (t, 0, 0, 0, 0)),
                       pl.BlockSpec(c_init.shape, lambda t: (0, 0, 0, 0))),
        )(h_pairs, c_pairs)

    return jax.shard_map(local_run, mesh=mesh, in_specs=(frame_spec, P(), P(), P(), state_spec, state_spec),
                         out_specs=(frame_spec, state_spec), check_vma=False)
```

```python
import functools

import jax
import jax.numpy as jnp
from jax import lax
from jax.experimental import pallas as pl
from jax.experimental.pallas import tpu as pltpu
from jax.sharding import PartitionSpec as P

MESH = pl.DeviceIdType.MESH
F32, BF16 = jnp.float32, jnp.bfloat16

DEPTH = 3
STEPS = 12
BLOCKS = STEPS // DEPTH
PAIRS = 16
OWN = 64
EDGE = 2
HP = -(-DEPTH // 2)
ROWS_ALL = PAIRS + 2 * EDGE
SUBL = 88
FROM_UP, FROM_DOWN, FROM_SIDE_A, FROM_SIDE_B, FROM_DUP, FROM_DDOWN = range(6)
MIRROR = (FROM_DOWN, FROM_UP, FROM_SIDE_A, FROM_SIDE_B, FROM_DDOWN, FROM_DUP)


def region(j):
    halo = DEPTH - 1 - j
    extra = -(-halo // 2)
    return EDGE - extra, PAIRS + 2 * extra, 72 if halo else OWN


def kernel(frames, wx_hbm, wh_hbm, bias_hbm, h_hbm, c_hbm, h_out, c_out,
           fbuf, wx_in, wh_in, bias_in, h_in, c_in, xs, hs, cs, xg, lhs, gts, wx, wh, bias,
           sx_row, sx_col, sx_cor, sh_row, sh_col, sh_cor, sc_row, sc_col, sc_cor,
           rx_row, rx_col, rx_cor, rh_row, rh_col, rh_cor, rc_row, rc_col, rc_cor,
           fsem, isem, ssem, rsem):
    row, col, grp = lax.axis_index("rows"), lax.axis_index("cols"), lax.axis_index("batch")
    n_rows = 4
    side = 1 - col
    has_up, has_down = row > 0, row < n_rows - 1
    peers = {
        FROM_UP: (has_up, row - 1, col),
        FROM_DOWN: (has_down, row + 1, col),
        FROM_SIDE_A: (None, row, side),
        FROM_SIDE_B: (None, row, side),
        FROM_DUP: (has_up, row - 1, side),
        FROM_DDOWN: (has_down, row + 1, side),
    }

    def guarded(cond, fn):
        if cond is None:
            fn()
        else:
            pl.when(cond)(fn)

    lane = lax.broadcasted_iota(jnp.int32, (72, 128), 1)
    subl = lax.broadcasted_iota(jnp.int32, (8, 128), 0)
    col_mask = jnp.where((subl + 2 * (1 - col) >= 2) & (subl < 6 + 2 * col), 1.0, 0.0).astype(F32)
    up_mask = jnp.where(has_up, 1.0, 0.0).astype(F32)
    down_mask = jnp.where(has_down, 1.0, 0.0).astype(F32)

    def frame_copy(t, slot):
        return pltpu.make_async_copy(frames.at[t], fbuf.at[slot], fsem.at[slot])

    for j in range(DEPTH):
        frame_copy(j, j).start()

    inputs = [pltpu.make_async_copy(src, dst, isem.at[i]) for i, (src, dst) in enumerate(
        ((h_hbm, h_in), (c_hbm, c_in), (wx_hbm, wx_in), (wh_hbm, wh_in), (bias_hbm, bias_in)))]
    for cp in inputs:
        cp.start()

    barrier = pltpu.get_barrier_semaphore()
    for d, (cond, r, c) in peers.items():
        if d == FROM_SIDE_B:
            continue
        guarded(cond, lambda r=r, c=c: pl.semaphore_signal(barrier, inc=1, device_id=(grp, c, r), device_id_type=MESH))

    def ingest(load, dst):
        def body(i, _):
            for u in range(4):
                q = i * 4 + u
                for s in range(2):
                    both = jnp.concatenate([load(s, 2 * q), load(s, 2 * q + 1)], axis=1).astype(F32)
                    dst[q, pl.ds(s, 32, stride=2), :] = both
            return 0
        lax.fori_loop(0, PAIRS // 4, body, 0)

    def wrap_first(ref, q):
        ref[q, 80:88, :] = ref[q, 8:16, :]

    nil = jnp.zeros((SUBL, 128), F32)
    for q in (0, 1, ROWS_ALL - 2, ROWS_ALL - 1):
        hs[q] = nil
        for j in range(DEPTH):
            xs[j, q] = nil
    for q in (0, PAIRS + 1):
        cs[q] = nil[0:72]
    for q in range(PAIRS):
        cs[1 + q, 64:72, :] = nil[0:8]

    strip_at = pl.multiple_of(8 + 56 * (1 - col), 8)
    cstrip_at = pl.multiple_of(56 * (1 - col), 8)
    cstrip_from = pl.multiple_of(60 * (1 - col), 4)
    cstrip_to = pl.multiple_of(64 + 4 * col, 4)

    def pack_rows(src, s_row):
        for p in range(HP):
            s_row[0, p] = src[EDGE + p, 8:72, :].astype(BF16)
            s_row[1, p] = src[EDGE + PAIRS - HP + p, 8:72, :].astype(BF16)

    def pack_cols(src, s_col, s_cor, part):
        for i in range(4 * part, 4 * part + 4):
            two = jnp.concatenate([src[EDGE + 2 * i, pl.ds(strip_at, 8), :],
                                   src[EDGE + 2 * i + 1, pl.ds(strip_at, 8), :]], axis=0).astype(BF16)
            s_col[i] = two
            if i == 0:
                s_cor[0] = two
            if i == PAIRS // 2 - 1:
                s_cor[1] = two

    def unpack_side(dst, q, strip):
        strip = strip * col_mask
        dst[q, 72:80, :] = strip
        dst[q, 0:8, :] = strip

    def unpack_bf16(dst, get_row, get_col, get_cor):
        for i in range(PAIRS // 2):
            both = get_col(i).astype(F32)
            unpack_side(dst, EDGE + 2 * i, both[0:8])
            unpack_side(dst, EDGE + 2 * i + 1, both[8:16])

        def rows(which, first):
            for p in range(HP):
                strip = get_row(which, p).astype(F32)
                dst[first + p, 8:72, :] = strip
                dst[first + p, 80:88, :] = strip[0:8]
            both = get_cor(which).astype(F32)
            for p in range(HP):
                at = 2 - HP + p if which == 0 else p
                unpack_side(dst, first + p, both[8 * at:8 * at + 8])

        pl.when(has_up)(lambda: rows(0, EDGE - HP))
        pl.when(has_down)(lambda: rows(1, EDGE + PAIRS))

    def copies(b, kind, dirs, arriving=False):
        (s_row, s_col, s_cor), (r_row, r_col, r_cor) = bufs(b, kind)
        out = {}
        for d in dirs:
            cond, r, c = peers[d]
            m = d if arriving else MIRROR[d]
            if d in (FROM_UP, FROM_DOWN):
                src, dst = s_row.at[d], r_row.at[m]
            elif d in (FROM_SIDE_A, FROM_SIDE_B):
                half = pl.ds(4 * (d - FROM_SIDE_A), 4)
                src, dst = s_col.at[half], r_col.at[half]
            else:
                src, dst = s_cor.at[d - FROM_DUP], r_cor.at[m - FROM_DUP]
            out[d] = (cond, pltpu.make_async_remote_copy(
                src_ref=src, dst_ref=dst, send_sem=ssem.at[b, kind, d], recv_sem=rsem.at[b, kind, m],
                device_id=(grp, c, r), device_id_type=MESH))
        return out

    def bufs(b, kind):
        if kind < DEPTH:
            return ((sx_row.at[b, kind], sx_col.at[b, kind], sx_cor.at[b, kind]),
                    (rx_row.at[b, kind], rx_col.at[b, kind], rx_cor.at[b, kind]))
        if kind == DEPTH:
            return ((sh_row.at[b], sh_col.at[b], sh_cor.at[b]), (rh_row.at[b], rh_col.at[b], rh_cor.at[b]))
        return ((sc_row.at[b], sc_col.at[b], sc_cor.at[b]), (rc_row.at[b], rc_col.at[b], rc_cor.at[b]))

    OTHERS = (FROM_UP, FROM_DOWN, FROM_DUP, FROM_DDOWN)

    def send(b, kind, dirs):
        for cond, cp in copies(b, kind, dirs).values():
            guarded(cond, lambda cp=cp: cp.start())

    def receive(b, kind):
        for cond, cp in copies(b, kind, peers, arriving=True).values():
            guarded(cond, lambda cp=cp: cp.wait_recv())

    def send_state_cols(b, part):
        pack_cols(hs, sh_col.at[b], sh_cor.at[b], part)
        for q in range(8 * part, 8 * part + 8):
            sc_col[b, q // 2, 4 * (q % 2):4 * (q % 2) + 4] = cs[1 + q, pl.ds(cstrip_from, 4), :]
        for kind in (DEPTH, DEPTH + 1):
            send(b, kind, (FROM_SIDE_A + part,))

    def send_state_rest(b):
        pack_rows(hs, sh_row.at[b])
        sc_row[b, 0] = cs[1, 0:OWN, :]
        sc_row[b, 1] = cs[PAIRS, 0:OWN, :]
        sc_cor[b, 0] = cs[1, pl.ds(cstrip_at, 8), :]
        sc_cor[b, 1] = cs[PAIRS, pl.ds(cstrip_at, 8), :]
        for kind in (DEPTH, DEPTH + 1):
            send(b, kind, OTHERS)

    def receive_state(b):
        receive(b, DEPTH)
        unpack_bf16(hs, lambda w, p: rh_row[b, w, p], lambda i: rh_col[b, i], lambda w: rh_cor[b, w])
        if DEPTH > 1:
            receive(b, DEPTH + 1)
            for q in range(PAIRS):
                cs[1 + q, pl.ds(cstrip_to, 4), :] = rc_col[b, q // 2, 4 * (q % 2):4 * (q % 2) + 4]

            def rows(which, at):
                cs[at, 0:OWN, :] = rc_row[b, which]
                cs[at, 64:72, :] = rc_cor[b, which]

            pl.when(has_up)(lambda: rows(0, 0))
            pl.when(has_down)(lambda: rows(1, 1 + PAIRS))

    def take_frame(b, j, pairs):
        for q in pairs:
            for s in range(2):
                both = jnp.concatenate([fbuf[j, s, 2 * q], fbuf[j, s, 2 * q + 1]], axis=1).astype(F32)
                xs[j, EDGE + q, pl.ds(8 + s, 32, stride=2), :] = both
            wrap_first(xs.at[j], EDGE + q)

    def pack_frame(b, j):
        pack_rows(xs.at[j], sx_row.at[b, j])
        for part in range(2):
            pack_cols(xs.at[j], sx_col.at[b, j], sx_cor.at[b, j], part)

    def tasks(j):
        first, count, width = region(j)
        n = 6 if count == 18 else 8
        return [(j, first + g, n, width, g * width) for g in range(0, count, n)]

    def build(src, slot, task):
        _, first, n, width, _ = task
        low = (lane < 64)[0:width]
        for q in range(0, n, 2):
            for dx in range(3):
                at = pl.ds(6 + 2 * dx, width)
                r = [src[first + q + i, at, :] for i in range(-1, 3)]
                own = jnp.concatenate([r[1], r[2]], axis=0).astype(BF16)
                near = jnp.concatenate([jnp.where(low, r[2], r[0]), jnp.where(low, r[3], r[1])], axis=0).astype(BF16)
                lhs[slot, q * width:(q + 2) * width, dx * 256:dx * 256 + 128] = own
                lhs[slot, q * width:(q + 2) * width, dx * 256 + 128:dx * 256 + 256] = near

    def product(slot, task, w):
        _, _, n, width, _ = task
        return jnp.dot(lhs[slot, 0:n * width, :], w[...], preferred_element_type=F32)

    def conv_x(b, following, early=False):
        def arrive(j):
            receive(b, j)
            unpack_bf16(xs.at[j], lambda w, p: rx_row[b, j, w, p], lambda i: rx_col[b, j, i], lambda w: rx_cor[b, j, w])

        for j in range(1 if early else DEPTH):
            arrive(j)

        @pl.when(following < BLOCKS)
        def _():
            for j in range(DEPTH):
                frame_copy(0, j).wait()

        todo = [t for j in range(DEPTH) for t in tasks(j)]
        build(xs.at[0], 0, todo[0])
        for i, task in enumerate(todo):
            if i + 1 < len(todo):
                if early and todo[i + 1][0] != task[0]:
                    arrive(todo[i + 1][0])
                build(xs.at[todo[i + 1][0]], (i + 1) % 2, todo[i + 1])
            j, _, n, width, at = task
            xg[j, at:at + n * width, :] = product(i % 2, task, wx) + bias[...]
            if i + 1 == len(todo) or todo[i + 1][0] != j:
                take_frame(following, j, range(PAIRS))
                pack_frame(following, j)

        @pl.when(following < BLOCKS)
        def _():
            for j in range(DEPTH):
                send(following, j, peers)

        @pl.when(following + 1 < BLOCKS)
        def _():
            for j in range(DEPTH):
                frame_copy((following + 1) * DEPTH + j, j).start()

    def cells(slot, task, t):
        j, first, n, width, base = task
        gts[slot, 0:n * width, :] = product(slot, task, wh) + xg[j, base:base + n * width, :]
        for q in range(n):
            rows_q = pl.ds(q * width, width)
            gi, gf, go, gg = (gts[slot, rows_q, 128 * i:128 * i + 128] for i in range(4))
            at = first + q
            c_old = cs[at - 1, 0:width, :]
            ti, tf, to = jnp.tanh(0.5 * gi), jnp.tanh(0.5 * gf), jnp.tanh(0.5 * go)
            c_new = 0.5 * ((tf + 1.0) * c_old + (ti + 1.0) * jnp.tanh(gg))
            cs[at - 1, 0:width, :] = c_new
            h_new = 0.5 * (to + 1.0) * jnp.tanh(c_new)
            if at < EDGE:
                h_new = h_new * up_mask
            if at >= EDGE + PAIRS:
                h_new = h_new * down_mask
            hs[at, 8:72, :] = h_new[0:OWN]
            hs[at, 80:88, :] = h_new[0:8]
            if width == 72:
                unpack_side(hs, at, h_new[64:72])
            if EDGE <= at < EDGE + PAIRS:
                for s in range(2):
                    both = hs[at, pl.ds(8 + s, 32, stride=2), :].astype(BF16)
                    h_out[t, s, 2 * (at - EDGE)] = both[:, 0:64]
                    h_out[t, s, 2 * (at - EDGE) + 1] = both[:, 64:128]

    def steps(b, sends):
        todo = [t for j in range(DEPTH) for t in tasks(j)]
        build(hs, 0, todo[0])
        for i, task in enumerate(todo):
            if i + 1 < len(todo):
                build(hs, (i + 1) % 2, todo[i + 1])
            cells(i % 2, task, b * DEPTH + task[0])
            if sends and i + 2 >= len(todo):
                send_state_cols(b + 1, i + 2 - len(todo))
        if sends:
            send_state_rest(b + 1)

    def weights(src, dst):
        zero = jnp.zeros((64, 64), BF16)
        for dx in range(3):
            for k, q in enumerate((0, 1, 2, -1)):
                for g in range(4):
                    parts = []
                    for p in range(2):
                        dy = q - p + 1
                        parts.append(src[dy, dx, :, 64 * g:64 * g + 64] if 0 <= dy <= 2 else zero)
                    dst[dx * 256 + k * 64:dx * 256 + k * 64 + 64, 128 * g:128 * g + 128] = jnp.concatenate(parts, axis=1)

    count = 3 + 2 * (has_up & has_down).astype(jnp.int32)
    for j in range(DEPTH):
        frame_copy(0, j).wait()
        take_frame(0, j, range(PAIRS))
        pack_frame(0, j)
        if j == 0:
            pl.semaphore_wait(barrier, count)
        send(0, j, peers)
    for j in range(DEPTH):
        frame_copy(DEPTH + j, j).start()
    for cp in inputs:
        cp.wait()
    ingest(lambda s, r: h_in[s, r], hs.at[pl.ds(EDGE, PAIRS), pl.ds(8, OWN)])
    ingest(lambda s, r: c_in[s, r], cs.at[pl.ds(1, PAIRS), pl.ds(0, OWN)])
    for q in range(PAIRS):
        wrap_first(hs, EDGE + q)
    for part in range(2):
        send_state_cols(0, part)
    send_state_rest(0)
    weights(wx_in, wx)
    weights(wh_in, wh)
    for g in range(4):
        piece = bias_in[:, 64 * g:64 * g + 64]
        bias[:, 128 * g:128 * g + 128] = jnp.concatenate([piece, piece], axis=1)
    conv_x(0, 1, early=True)

    def block(b, _):
        receive_state(b)
        steps(b, True)
        conv_x(b + 1, b + 2)
        return 0

    lax.fori_loop(0, BLOCKS - 1, block, 0)
    receive_state(BLOCKS - 1)
    steps(BLOCKS - 1, False)

    for q in range(PAIRS):
        for s in range(2):
            both = cs[1 + q, pl.ds(s, 32, stride=2), :]
            c_out[s, 2 * q] = both[:, 0:64]
            c_out[s, 2 * q + 1] = both[:, 64:128]

    def drain(b, _):
        for kind in range(DEPTH + 2):
            for cond, cp in copies(b, kind, peers).values():
                guarded(cond, lambda cp=cp: cp.wait_send())
        return 0

    lax.fori_loop(0, BLOCKS, drain, 0)


def write_out(h, c, h_out, c_out, sem):
    copies = [pltpu.make_async_copy(h.at[t], h_out.at[t], sem.at[t]) for t in range(STEPS)]
    copies.append(pltpu.make_async_copy(c, c_out, sem.at[STEPS]))
    for cp in copies:
        cp.start()
    for cp in copies:
        cp.wait()


def solution(mesh):
    frame_spec = P(None, "batch", "rows", "cols", None)
    state_spec = P("batch", "rows", "cols", None)

    def local_run(frames, w_x, w_h, gate_bias, h_init, c_init):
        vmem = pl.BlockSpec(memory_space=pltpu.VMEM)
        hbm = pl.BlockSpec(memory_space=pltpu.HBM)
        most = max(region(j)[1] * region(j)[2] for j in range(DEPTH))
        strips = [
            [(BLOCKS, DEPTH, 2, HP, OWN, 128), (BLOCKS, DEPTH, 8, 16, 128), (BLOCKS, DEPTH, 2, 16, 128)],
            [(BLOCKS, 2, HP, OWN, 128), (BLOCKS, 8, 16, 128), (BLOCKS, 2, 16, 128)],
            [(BLOCKS, 2, OWN, 128), (BLOCKS, PAIRS // 2, 8, 128), (BLOCKS, 2, 8, 128)],
        ]
        recv_bufs = [pltpu.VMEM(s, BF16 if k < 2 else F32) for k in range(3) for s in strips[k]]
        strips[0] = [(s[0] + 1,) + s[1:] for s in strips[0]]
        send_bufs = [pltpu.VMEM(s, BF16 if k < 2 else F32) for k in range(3) for s in strips[k]]
        h_pairs, c_pairs = pl.pallas_call(
            kernel,
            out_shape=(pltpu.VMEM(frames.shape, BF16), pltpu.VMEM(c_init.shape, F32)),
            in_specs=[hbm] * 6,
            out_specs=(vmem, vmem),
            scratch_shapes=[
                pltpu.VMEM((DEPTH,) + h_init.shape, BF16),
                pltpu.VMEM(w_x.shape, BF16),
                pltpu.VMEM(w_h.shape, BF16),
                pltpu.VMEM((1, 256), F32),
                pltpu.VMEM(h_init.shape, BF16),
                pltpu.VMEM(c_init.shape, F32),
                pltpu.VMEM((DEPTH, ROWS_ALL, SUBL, 128), F32),
                pltpu.VMEM((ROWS_ALL, SUBL, 128), F32),
                pltpu.VMEM((PAIRS + 2, 72, 128), F32),
                pltpu.VMEM((DEPTH, most, 512), F32),
                pltpu.VMEM((2, 512, 768), BF16),
                pltpu.VMEM((2, 512, 512), F32),
                pltpu.VMEM((768, 512), BF16),
                pltpu.VMEM((768, 512), BF16),
                pltpu.VMEM((1, 512), F32),
                *send_bufs, *recv_bufs,
                pltpu.SemaphoreType.DMA((DEPTH,)),
                pltpu.SemaphoreType.DMA((5,)),
                pltpu.SemaphoreType.DMA((BLOCKS, DEPTH + 2, 6)),
                pltpu.SemaphoreType.DMA((BLOCKS, DEPTH + 2, 6)),
            ],
            compiler_params=pltpu.CompilerParams(collective_id=0, has_side_effects=True, vmem_limit_bytes=56 * 2**20),
        )(frames, w_x, w_h, gate_bias.reshape(1, 256), h_init, c_init)
        return pl.pallas_call(
            write_out,
            out_shape=(jax.ShapeDtypeStruct(frames.shape, BF16), jax.ShapeDtypeStruct(c_init.shape, F32)),
            in_specs=[vmem, vmem],
            out_specs=(hbm, hbm),
            scratch_shapes=[pltpu.SemaphoreType.DMA((STEPS + 1,))],
            compiler_params=pltpu.CompilerParams(vmem_limit_bytes=16 * 2**20),
        )(h_pairs, c_pairs)

    return jax.shard_map(local_run, mesh=mesh, in_specs=(frame_spec, P(), P(), P(), state_spec, state_spec),
                         out_specs=(frame_spec, state_spec), check_vma=False)
```

```python
import functools

import jax
import jax.numpy as jnp
from jax import lax
from jax.experimental import pallas as pl
from jax.experimental.pallas import tpu as pltpu
from jax.sharding import PartitionSpec as P

MESH = pl.DeviceIdType.MESH
F32, BF16 = jnp.float32, jnp.bfloat16

DEPTH = 3
STEPS = 12
BLOCKS = STEPS // DEPTH
PAIRS = 16
OWN = 64
EDGE = 2
HP = -(-DEPTH // 2)
ROWS_ALL = PAIRS + 2 * EDGE
SUBL = 88
FROM_UP, FROM_DOWN, FROM_SIDE, FROM_DUP, FROM_DDOWN = DIRS = range(5)
MIRROR = (FROM_DOWN, FROM_UP, FROM_SIDE, FROM_DDOWN, FROM_DUP)
FRAME, HID, CELL = range(3)


def region(j):
    halo = DEPTH - 1 - j
    extra = -(-halo // 2)
    return EDGE - extra, PAIRS + 2 * extra, 72 if halo else OWN


def kernel(frames, wx_hbm, wh_hbm, bias_hbm, h_hbm, c_hbm, h_out, c_out,
           fbuf, wx_in, wh_in, bias_in, h_in, c_in, xs, hs, cs, xg, gts, wx, wh, bias,
           sx_row, sx_col, sx_cor, sh_row, sh_col, sh_cor, sc_row, sc_col, sc_cor,
           rx_row, rx_col, rx_cor, rh_row, rh_col, rh_cor, rc_row, rc_col, rc_cor,
           fsem, isem, ssem, rsem):
    row, col, grp = lax.axis_index("rows"), lax.axis_index("cols"), lax.axis_index("batch")
    n_rows = lax.axis_size("rows")
    side = 1 - col
    has_up, has_down = row > 0, row < n_rows - 1
    above, below = lax.rem(row + n_rows - 1, n_rows), lax.rem(row + 1, n_rows)
    peers = ((above, col), (below, col), (row, side), (above, side), (below, side))

    lane = lax.broadcasted_iota(jnp.int32, (72, 128), 1)
    subl = lax.broadcasted_iota(jnp.int32, (8, 128), 0)
    col_mask = jnp.where((subl + 2 * (1 - col) >= 2) & (subl < 6 + 2 * col), 1.0, 0.0).astype(F32)
    up_mask = jnp.where(has_up, 1.0, 0.0).astype(F32)
    down_mask = jnp.where(has_down, 1.0, 0.0).astype(F32)

    def frame_copy(t, slot):
        return pltpu.make_async_copy(frames.at[t], fbuf.at[slot], fsem.at[slot])

    for j in range(DEPTH):
        frame_copy(j, j).start()

    inputs = [pltpu.make_async_copy(src, dst, isem.at[i]) for i, (src, dst) in enumerate(
        ((h_hbm, h_in), (c_hbm, c_in), (wx_hbm, wx_in), (wh_hbm, wh_in), (bias_hbm, bias_in)))]
    for cp in inputs:
        cp.start()

    barrier = pltpu.get_barrier_semaphore()
    for r, c in peers:
        pl.semaphore_signal(barrier, inc=1, device_id=(grp, c, r), device_id_type=MESH)

    def ingest(load, dst):
        def body(i, _):
            for u in range(4):
                q = i * 4 + u
                for s in range(2):
                    both = jnp.concatenate([load(s, 2 * q), load(s, 2 * q + 1)], axis=1).astype(F32)
                    dst[q, pl.ds(s, 32, stride=2), :] = both
            return 0
        lax.fori_loop(0, PAIRS // 4, body, 0)

    def wrap_first(ref, q):
        ref[q, 80:88, :] = ref[q, 8:16, :]

    nil = jnp.zeros((SUBL, 128), F32)
    for q in (0, 1, ROWS_ALL - 2, ROWS_ALL - 1):
        hs[q] = nil
        for j in range(DEPTH):
            xs[j, q] = nil
    for q in (0, PAIRS + 1):
        cs[q] = nil[0:72]
    for q in range(PAIRS):
        cs[1 + q, 64:72, :] = nil[0:8]

    strip_at = pl.multiple_of(8 + 56 * (1 - col), 8)
    cstrip_at = pl.multiple_of(56 * (1 - col), 8)
    cstrip_from = pl.multiple_of(60 * (1 - col), 4)
    cstrip_to = pl.multiple_of(64 + 4 * col, 4)

    def pack_rows(src, s_row):
        for p in range(HP):
            s_row[0, p] = src[EDGE + p, 8:72, :].astype(BF16)
            s_row[1, p] = src[EDGE + PAIRS - HP + p, 8:72, :].astype(BF16)

    def pack_cols(src, s_col, s_cor, part):
        for i in range(4 * part, 4 * part + 4):
            two = jnp.concatenate([src[EDGE + 2 * i, pl.ds(strip_at, 8), :],
                                   src[EDGE + 2 * i + 1, pl.ds(strip_at, 8), :]], axis=0).astype(BF16)
            s_col[i] = two
            if i == 0:
                s_cor[0] = two
            if i == PAIRS // 2 - 1:
                s_cor[1] = two

    def unpack_side(dst, q, strip):
        strip = strip * col_mask
        dst[q, 72:80, :] = strip
        dst[q, 0:8, :] = strip

    def unpack_bf16(dst, get_row, get_col, get_cor):
        for i in range(PAIRS // 2):
            both = get_col(i).astype(F32)
            unpack_side(dst, EDGE + 2 * i, both[0:8])
            unpack_side(dst, EDGE + 2 * i + 1, both[8:16])

        for which, first, mask in ((0, EDGE - HP, up_mask), (1, EDGE + PAIRS, down_mask)):
            both = get_cor(which).astype(F32) * mask
            for p in range(HP):
                strip = get_row(which, p).astype(F32) * mask
                dst[first + p, 8:72, :] = strip
                dst[first + p, 80:88, :] = strip[0:8]
                at = 2 - HP + p if which == 0 else p
                unpack_side(dst, first + p, both[8 * at:8 * at + 8])

    def ends(sends, recvs, d, m):
        (s_row, s_col, s_cor), (r_row, r_col, r_cor) = sends, recvs
        if d in (FROM_UP, FROM_DOWN):
            return s_row.at[d], r_row.at[m]
        if d == FROM_SIDE:
            return s_col, r_col
        return s_cor.at[d - FROM_DUP], r_cor.at[m - FROM_DUP]

    def remote(kind, b, j, d, m, src, dst):
        r, c = peers[d]
        return pltpu.make_async_remote_copy(
            src_ref=src, dst_ref=dst, send_sem=ssem.at[kind, d], recv_sem=rsem.at[b, kind + j, m],
            device_id=(grp, c, r), device_id_type=MESH)

    send_bufs = ((sx_row, sx_col, sx_cor), (sh_row, sh_col, sh_cor), (sc_row, sc_col, sc_cor))
    recv_bufs = ((rx_row, rx_col, rx_cor), (rh_row, rh_col, rh_cor), (rc_row, rc_col, rc_cor))

    def frame_sem(b, j):
        return 3 + j if isinstance(b, int) and b == 0 else 0

    def send_frame(b, j):
        for d in DIRS:
            sends, recvs = ([x.at[b, j] for x in bufs[FRAME]] for bufs in (send_bufs, recv_bufs))
            src, dst = ends(sends, recvs, d, MIRROR[d])
            remote(FRAME, b, frame_sem(b, j), d, MIRROR[d], src, dst).start()

    def receive_frames(b, j=None):
        for d in DIRS:
            if j is None:
                at = (b, slice(None), d) if d < FROM_SIDE else (b,) if d == FROM_SIDE else (b, slice(None), d - FROM_DUP)
            else:
                at = (b, j, d) if d < FROM_SIDE else (b, j) if d == FROM_SIDE else (b, j, d - FROM_DUP)
            which = 0 if d < FROM_SIDE else 1 if d == FROM_SIDE else 2
            remote(FRAME, b, frame_sem(b, j or 0), d, d, send_bufs[FRAME][which].at[at], recv_bufs[FRAME][which].at[at]).wait_recv()

    def send_state(kind, b, d, half=None):
        sends, recvs = ([x.at[b] for x in bufs[kind]] for bufs in (send_bufs, recv_bufs))
        src, dst = ends(sends, recvs, d, MIRROR[d])
        if half is not None:
            src, dst = src.at[pl.ds(4 * half, 4)], dst.at[pl.ds(4 * half, 4)]
        remote(kind, b, 0, d, MIRROR[d], src, dst).start()

    def receive_strips(b):
        for kind in (HID, CELL):
            for d in DIRS:
                sends, recvs = ([x.at[b] for x in bufs[kind]] for bufs in (send_bufs, recv_bufs))
                src, dst = ends(sends, recvs, d, d)
                remote(kind, b, 0, d, d, src, dst).wait_recv()

    def drain():
        for kind in (FRAME, HID, CELL):
            for d in DIRS:
                which = 0 if d < FROM_SIDE else 1 if d == FROM_SIDE else 2
                buf = send_bufs[kind][which]
                at = [pl.ds(0, BLOCKS)] + ([slice(None)] if kind == FRAME else [])
                if d != FROM_SIDE:
                    at.append(d if d < FROM_SIDE else d - FROM_DUP)
                whole, there = buf.at[tuple(at)], recv_bufs[kind][which].at[tuple(at)]
                remote(kind, 0, 0, d, d, whole, there).wait_send()

    def send_state_cols(b, part):
        pack_cols(hs, sh_col.at[b], sh_cor.at[b], part)
        for q in range(8 * part, 8 * part + 8):
            sc_col[b, q // 2, 4 * (q % 2):4 * (q % 2) + 4] = cs[1 + q, pl.ds(cstrip_from, 4), :]
        for kind in (HID, CELL):
            send_state(kind, b, FROM_SIDE, part)

    def send_state_rest(b):
        pack_rows(hs, sh_row.at[b])
        sc_row[b, 0] = cs[1, 0:OWN, :]
        sc_row[b, 1] = cs[PAIRS, 0:OWN, :]
        sc_cor[b, 0] = cs[1, pl.ds(cstrip_at, 8), :]
        sc_cor[b, 1] = cs[PAIRS, pl.ds(cstrip_at, 8), :]
        for kind in (HID, CELL):
            for d in (FROM_UP, FROM_DOWN, FROM_DUP, FROM_DDOWN):
                send_state(kind, b, d)

    def receive_state(b):
        receive_strips(b)
        unpack_bf16(hs, lambda w, p: rh_row[b, w, p], lambda i: rh_col[b, i], lambda w: rh_cor[b, w])
        for q in range(PAIRS):
            cs[1 + q, pl.ds(cstrip_to, 4), :] = rc_col[b, q // 2, 4 * (q % 2):4 * (q % 2) + 4]
        for which, at in ((0, 0), (1, 1 + PAIRS)):
            cs[at, 0:OWN, :] = rc_row[b, which]
            cs[at, 64:72, :] = rc_cor[b, which]

    def take_frame(b, j, pairs):
        for q in pairs:
            for s in range(2):
                both = jnp.concatenate([fbuf[j, s, 2 * q], fbuf[j, s, 2 * q + 1]], axis=1).astype(F32)
                xs[j, EDGE + q, pl.ds(8 + s, 32, stride=2), :] = both
            wrap_first(xs.at[j], EDGE + q)

    def pack_frame(b, j):
        pack_rows(xs.at[j], sx_row.at[b, j])
        for part in range(2):
            pack_cols(xs.at[j], sx_col.at[b, j], sx_cor.at[b, j], part)

    def tasks(j):
        first, count, width = region(j)
        n = 6 if count == 18 else 8
        return [(j, first + g, n, width, g * width) for g in range(0, count, n)]

    def product(src, task, w):
        _, first, n, width, _ = task
        low = (lane < 64)[0:width]
        total = None
        for dx in range(3):
            at = pl.ds(6 + 2 * dx, width)
            r = [src[first + i, at, :] for i in range(-1, n + 1)]
            own = jnp.concatenate(r[1:n + 1], axis=0).astype(BF16)
            near = jnp.concatenate([jnp.where(low, r[i + 2], r[i]) for i in range(n)], axis=0).astype(BF16)
            part = jnp.dot(jnp.concatenate([own, near], axis=1), w[dx * 256:dx * 256 + 256, :], preferred_element_type=F32)
            total = part if total is None else total + part
        return total

    def unpack_frame(b, j):
        unpack_bf16(xs.at[j], lambda w, p: rx_row[b, j, w, p], lambda i: rx_col[b, j, i], lambda w: rx_cor[b, j, w])

    def x_gates(src, slot, task):
        j, _, n, width, at = task
        xg[j, at:at + n * width, :] = product(src, task, wx) + bias[...]

    all_tasks = [t for j in range(DEPTH) for t in tasks(j)]
    last_of_step = [i + 1 == len(all_tasks) or all_tasks[i + 1][0] != t[0] for i, t in enumerate(all_tasks)]

    def frames_wait(following):
        for j in range(DEPTH):
            frame_copy(0, j).wait()

    def frames_on(following):
        def sends():
            for j in range(DEPTH):
                send_frame(following, j)

        def fetches():
            for j in range(DEPTH):
                frame_copy((following + 1) * DEPTH + j, j).start()

        if isinstance(following, int):
            sends()
            fetches()
        else:
            pl.when(following < BLOCKS)(sends)
            pl.when(following + 1 < BLOCKS)(fetches)

    def h_gates(src, slot, task):
        j, _, n, width, base = task
        gts[slot, 0:n * width, :] = product(src, task, wh) + xg[j, base:base + n * width, :]

    def cells(slot, task, t):
        j, first, n, width, base = task
        for q in range(n):
            rows_q = pl.ds(q * width, width)
            gi, gf, go, gg = (gts[slot, rows_q, 128 * i:128 * i + 128] for i in range(4))
            at = first + q
            c_old = cs[at - 1, 0:width, :]
            ti, tf, to = jnp.tanh(0.5 * gi), jnp.tanh(0.5 * gf), jnp.tanh(0.5 * go)
            c_new = 0.5 * ((tf + 1.0) * c_old + (ti + 1.0) * jnp.tanh(gg))
            cs[at - 1, 0:width, :] = c_new
            h_new = 0.5 * (to + 1.0) * jnp.tanh(c_new)
            if at < EDGE:
                h_new = h_new * up_mask
            if at >= EDGE + PAIRS:
                h_new = h_new * down_mask
            hs[at, 8:72, :] = h_new[0:OWN]
            hs[at, 80:88, :] = h_new[0:8]
            if width == 72:
                unpack_side(hs, at, h_new[64:72])
            if EDGE <= at < EDGE + PAIRS:
                for s in range(2):
                    both = hs[at, pl.ds(8 + s, 32, stride=2), :].astype(BF16)
                    h_out[t, s, 2 * (at - EDGE)] = both[:, 0:64]
                    h_out[t, s, 2 * (at - EDGE) + 1] = both[:, 64:128]

    def run(hid_block, x_block):
        todo = []
        if hid_block is not None:
            todo += [(hs, t, True) for t in all_tasks]
        if x_block is not None:
            todo += [(xs.at[t[0]], t, False) for t in all_tasks]
        def ahead(i):
            src, task, hidden = todo[i]
            (h_gates if hidden else x_gates)(src, i % 2, task)

        ahead(0)
        for i, (src, task, hidden) in enumerate(todo):
            n = i % len(all_tasks)
            if hidden and x_block is not None and n + 1 == len(all_tasks):
                for j in range(DEPTH):
                    unpack_frame(x_block, j)
            if i + 1 < len(todo):
                ahead(i + 1)
            if hidden:
                cells(i % 2, task, hid_block * DEPTH + task[0])
                if x_block is not None:
                    if n + 2 >= len(all_tasks):
                        send_state_cols(hid_block + 1, n + 2 - len(all_tasks))
                    if n + 2 == len(all_tasks):
                        receive_frames(x_block)
                    if n + 1 == len(all_tasks):
                        send_state_rest(hid_block + 1)
            elif last_of_step[n]:
                take_frame(x_block + 1, task[0], range(PAIRS))
                pack_frame(x_block + 1, task[0])

    def weights(src, dst):
        zero = jnp.zeros((64, 64), BF16)
        for dx in range(3):
            for k, q in enumerate((0, 1, 2, -1)):
                for g in range(4):
                    parts = []
                    for p in range(2):
                        dy = q - p + 1
                        parts.append(src[dy, dx, :, 64 * g:64 * g + 64] if 0 <= dy <= 2 else zero)
                    dst[dx * 256 + k * 64:dx * 256 + k * 64 + 64, 128 * g:128 * g + 128] = jnp.concatenate(parts, axis=1)

    for j in range(DEPTH):
        frame_copy(0, j).wait()
        take_frame(0, j, range(PAIRS))
        pack_frame(0, j)
        if j == 0:
            pl.semaphore_wait(barrier, len(peers))
        send_frame(0, j)
    for j in range(DEPTH):
        frame_copy(DEPTH + j, j).start()
    for cp in inputs:
        cp.wait()
    ingest(lambda s, r: h_in[s, r], hs.at[pl.ds(EDGE, PAIRS), pl.ds(8, OWN)])
    ingest(lambda s, r: c_in[s, r], cs.at[pl.ds(1, PAIRS), pl.ds(0, OWN)])
    for q in range(PAIRS):
        wrap_first(hs, EDGE + q)
    for part in range(2):
        send_state_cols(0, part)
    send_state_rest(0)
    weights(wx_in, wx)
    weights(wh_in, wh)
    for g in range(4):
        piece = bias_in[:, 64 * g:64 * g + 64]
        bias[:, 128 * g:128 * g + 128] = jnp.concatenate([piece, piece], axis=1)
    for j in range(DEPTH):
        receive_frames(0, j)
        unpack_frame(0, j)
        if j == DEPTH - 1:
            frames_wait(1)
        for task in tasks(j):
            x_gates(xs.at[j], 0, task)
    for j in range(DEPTH):
        take_frame(1, j, range(PAIRS))
        pack_frame(1, j)
    frames_on(1)

    def block(b, _):
        pl.when(b + 2 < BLOCKS)(lambda: frames_wait(b + 2))
        receive_state(b)
        run(b, b + 1)
        frames_on(b + 2)
        return 0

    lax.fori_loop(0, BLOCKS - 1, block, 0)
    receive_state(BLOCKS - 1)
    run(BLOCKS - 1, None)

    for q in range(PAIRS):
        for s in range(2):
            both = cs[1 + q, pl.ds(s, 32, stride=2), :]
            c_out[s, 2 * q] = both[:, 0:64]
            c_out[s, 2 * q + 1] = both[:, 64:128]

    drain()


def write_out(h, c, h_out, c_out, sem):
    copies = [pltpu.make_async_copy(h.at[t], h_out.at[t], sem.at[t]) for t in range(STEPS)]
    copies.append(pltpu.make_async_copy(c, c_out, sem.at[STEPS]))
    for cp in copies:
        cp.start()
    for cp in copies:
        cp.wait()


def solution(mesh):
    frame_spec = P(None, "batch", "rows", "cols", None)
    state_spec = P("batch", "rows", "cols", None)

    def local_run(frames, w_x, w_h, gate_bias, h_init, c_init):
        vmem = pl.BlockSpec(memory_space=pltpu.VMEM)
        hbm = pl.BlockSpec(memory_space=pltpu.HBM)
        most = max(region(j)[1] * region(j)[2] for j in range(DEPTH))
        strips = [
            [(BLOCKS, DEPTH, 2, HP, OWN, 128), (BLOCKS, DEPTH, 8, 16, 128), (BLOCKS, DEPTH, 2, 16, 128)],
            [(BLOCKS, 2, HP, OWN, 128), (BLOCKS, 8, 16, 128), (BLOCKS, 2, 16, 128)],
            [(BLOCKS, 2, OWN, 128), (BLOCKS, PAIRS // 2, 8, 128), (BLOCKS, 2, 8, 128)],
        ]
        recv_bufs = [pltpu.VMEM(s, BF16 if k < 2 else F32) for k in range(3) for s in strips[k]]
        strips[0] = [(s[0] + 1,) + s[1:] for s in strips[0]]
        send_bufs = [pltpu.VMEM(s, BF16 if k < 2 else F32) for k in range(3) for s in strips[k]]
        h_pairs, c_pairs = pl.pallas_call(
            kernel,
            out_shape=(pltpu.VMEM(frames.shape, BF16), pltpu.VMEM(c_init.shape, F32)),
            in_specs=[hbm] * 6,
            out_specs=(vmem, vmem),
            scratch_shapes=[
                pltpu.VMEM((DEPTH,) + h_init.shape, BF16),
                pltpu.VMEM(w_x.shape, BF16),
                pltpu.VMEM(w_h.shape, BF16),
                pltpu.VMEM((1, 256), F32),
                pltpu.VMEM(h_init.shape, BF16),
                pltpu.VMEM(c_init.shape, F32),
                pltpu.VMEM((DEPTH, ROWS_ALL, SUBL, 128), F32),
                pltpu.VMEM((ROWS_ALL, SUBL, 128), F32),
                pltpu.VMEM((PAIRS + 2, 72, 128), F32),
                pltpu.VMEM((DEPTH, most, 512), F32),
                pltpu.VMEM((2, 512, 512), F32),
                pltpu.VMEM((768, 512), BF16),
                pltpu.VMEM((768, 512), BF16),
                pltpu.VMEM((1, 512), F32),
                *send_bufs, *recv_bufs,
                pltpu.SemaphoreType.DMA((DEPTH,)),
                pltpu.SemaphoreType.DMA((5,)),
                pltpu.SemaphoreType.DMA((3, 5)),
                pltpu.SemaphoreType.DMA((BLOCKS, 3 + DEPTH, 5)),
            ],
            compiler_params=pltpu.CompilerParams(collective_id=0, has_side_effects=True, vmem_limit_bytes=56 * 2**20),
        )(frames, w_x, w_h, gate_bias.reshape(1, 256), h_init, c_init)
        return pl.pallas_call(
            write_out,
            out_shape=(jax.ShapeDtypeStruct(frames.shape, BF16), jax.ShapeDtypeStruct(c_init.shape, F32)),
            in_specs=[vmem, vmem],
            out_specs=(hbm, hbm),
            scratch_shapes=[pltpu.SemaphoreType.DMA((STEPS + 1,))],
            compiler_params=pltpu.CompilerParams(vmem_limit_bytes=16 * 2**20),
        )(h_pairs, c_pairs)

    return jax.shard_map(local_run, mesh=mesh, in_specs=(frame_spec, P(), P(), P(), state_spec, state_spec),
                         out_specs=(frame_spec, state_spec), check_vma=False)
```

```python
import functools

import jax
import jax.numpy as jnp
from jax import lax
from jax.experimental import pallas as pl
from jax.experimental.pallas import tpu as pltpu
from jax.sharding import PartitionSpec as P

MESH = pl.DeviceIdType.MESH
F32, BF16 = jnp.float32, jnp.bfloat16

DEPTH = 3
STEPS = 12
BLOCKS = STEPS // DEPTH
PAIRS = 16
OWN = 64
EDGE = 2
HP = -(-DEPTH // 2)
ROWS_ALL = PAIRS + 2 * EDGE
SUBL = 88
FROM_UP, FROM_DOWN, FROM_SIDE, FROM_DUP, FROM_DDOWN = DIRS = range(5)
MIRROR = (FROM_DOWN, FROM_UP, FROM_SIDE, FROM_DDOWN, FROM_DUP)
FRAME, HID, CELL = range(3)
COL_ORDER = (0, 1, 6, 7, 2, 3, 4, 5)


def region(j):
    halo = DEPTH - 1 - j
    extra = -(-halo // 2)
    return EDGE - extra, PAIRS + 2 * extra, 72 if halo else OWN


def kernel(frames, wx_hbm, wh_hbm, bias_hbm, h_hbm, c_hbm, h_out, c_out,
           fbuf, wx_in, wh_in, bias_in, h_in, c_in, xs, hs, cs, xg, gts, wx, wh, bias,
           sx_row, sx_col, sx_cor, sh_row, sh_col, sh_cor, sc_row, sc_col, sc_cor,
           rx_row, rx_col, rx_cor, rh_row, rh_col, rh_cor, rc_row, rc_col, rc_cor,
           fsem, isem, ssem, rsem):
    row, col, grp = lax.axis_index("rows"), lax.axis_index("cols"), lax.axis_index("batch")
    n_rows = lax.axis_size("rows")
    side = 1 - col
    has_up, has_down = row > 0, row < n_rows - 1
    above, below = lax.rem(row + n_rows - 1, n_rows), lax.rem(row + 1, n_rows)
    peers = ((above, col), (below, col), (row, side), (above, side), (below, side))

    lane = lax.broadcasted_iota(jnp.int32, (72, 128), 1)
    subl = lax.broadcasted_iota(jnp.int32, (8, 128), 0)
    col_mask = jnp.where((subl + 2 * (1 - col) >= 2) & (subl < 6 + 2 * col), 1.0, 0.0).astype(F32)
    up_mask = jnp.where(has_up, 1.0, 0.0).astype(F32)
    down_mask = jnp.where(has_down, 1.0, 0.0).astype(F32)

    def frame_copy(t, slot):
        return pltpu.make_async_copy(frames.at[t], fbuf.at[slot], fsem.at[slot])

    for j in range(DEPTH):
        frame_copy(j, j).start()

    inputs = [pltpu.make_async_copy(src, dst, isem.at[i]) for i, (src, dst) in enumerate(
        ((h_hbm, h_in), (c_hbm, c_in), (wx_hbm, wx_in), (wh_hbm, wh_in), (bias_hbm, bias_in)))]
    for cp in inputs:
        cp.start()

    barrier = pltpu.get_barrier_semaphore()
    def toward(fn):
        def both(a, b):
            fn(a)
            fn(b)

        fn(FROM_SIDE)
        pl.when(has_up)(lambda: both(FROM_UP, FROM_DUP))
        pl.when(has_down)(lambda: both(FROM_DOWN, FROM_DDOWN))

    toward(lambda d: pl.semaphore_signal(barrier, inc=1, device_id=(grp, peers[d][1], peers[d][0]), device_id_type=MESH))

    def ingest(load, dst):
        def body(i, _):
            for u in range(4):
                q = i * 4 + u
                for s in range(2):
                    both = jnp.concatenate([load(s, 2 * q), load(s, 2 * q + 1)], axis=1).astype(F32)
                    dst[q, pl.ds(s, 32, stride=2), :] = both
            return 0
        lax.fori_loop(0, PAIRS // 4, body, 0)

    def wrap_first(ref, q):
        ref[q, 80:88, :] = ref[q, 8:16, :]

    nil = jnp.zeros((SUBL, 128), F32)
    for q in (0, 1, ROWS_ALL - 2, ROWS_ALL - 1):
        hs[q] = nil
        for j in range(DEPTH):
            xs[j, q] = nil
    for q in (0, PAIRS + 1):
        cs[q] = nil[0:72]
    for q in range(PAIRS):
        cs[1 + q, 64:72, :] = nil[0:8]
        for j in range(1, DEPTH):
            xs[j, EDGE + q, 0:8, :] = nil[0:8]
            xs[j, EDGE + q, 72:80, :] = nil[0:8]

    strip_at = pl.multiple_of(8 + 56 * (1 - col), 8)
    cstrip_at = pl.multiple_of(56 * (1 - col), 8)
    cstrip_from = pl.multiple_of(60 * (1 - col), 4)
    cstrip_to = pl.multiple_of(64 + 4 * col, 4)

    def pack_rows(src, s_row):
        for p in range(HP):
            s_row[0, p] = src[EDGE + p, 8:72, :].astype(BF16)
            s_row[1, p] = src[EDGE + PAIRS - HP + p, 8:72, :].astype(BF16)

    def pack_cols(src, s_col, s_cor, part):
        for at, i in list(enumerate(COL_ORDER))[4 * part:4 * part + 4]:
            two = jnp.concatenate([src[EDGE + 2 * i, pl.ds(strip_at, 8), :],
                                   src[EDGE + 2 * i + 1, pl.ds(strip_at, 8), :]], axis=0).astype(BF16)
            s_col[at] = two
            if i == 0:
                s_cor[0] = two
            if i == PAIRS // 2 - 1:
                s_cor[1] = two

    def pack_narrow(src, s_row, s_col, s_cor):
        s_row[0, 0] = src[EDGE, 8:72, :].astype(BF16)
        s_row[1, 0] = src[EDGE + PAIRS - 1, 8:72, :].astype(BF16)
        for i in range(PAIRS // 4):
            s_col[i] = jnp.concatenate([src[EDGE + 4 * i + u, pl.ds(8 + cstrip_from, 4), :] for u in range(4)],
                                       axis=0).astype(BF16)
        for side_of, at in ((0, EDGE), (1, EDGE + PAIRS - 1)):
            edge = src[at, pl.ds(strip_at, 8), :]
            s_cor[side_of] = jnp.concatenate([edge, edge], axis=0).astype(BF16)

    def unpack_narrow(dst, get_row, get_col, get_cor):
        for i in range(PAIRS // 4):
            four = get_col(i).astype(F32)
            for u in range(4):
                strip = four[4 * u:4 * u + 4]
                dst[EDGE + 4 * i + u, pl.ds(8 + cstrip_to, 4), :] = strip
                dst[EDGE + 4 * i + u, pl.ds(cstrip_to - 64, 4), :] = strip
        for which, at, there in ((0, EDGE - 1, has_up), (1, EDGE + PAIRS, has_down)):
            strip = jnp.where(there, get_row(which).astype(F32), 0.0)
            dst[at, 8:72, :] = strip
            dst[at, 80:88, :] = strip[0:8]
            unpack_side(dst, at, jnp.where(there, get_cor(which).astype(F32)[0:8], 0.0))

    def unpack_side(dst, q, strip):
        strip = strip * col_mask
        dst[q, 72:80, :] = strip
        dst[q, 0:8, :] = strip

    def unpack_bf16(dst, get_row, get_col, get_cor):
        for at, i in enumerate(COL_ORDER):
            both = get_col(at).astype(F32)
            unpack_side(dst, EDGE + 2 * i, both[0:8])
            unpack_side(dst, EDGE + 2 * i + 1, both[8:16])

        for which, first, there in ((0, EDGE - HP, has_up), (1, EDGE + PAIRS, has_down)):
            both = jnp.where(there, get_cor(which).astype(F32), 0.0)
            for p in range(HP):
                strip = jnp.where(there, get_row(which, p).astype(F32), 0.0)
                dst[first + p, 8:72, :] = strip
                dst[first + p, 80:88, :] = strip[0:8]
                at = 2 - HP + p if which == 0 else p
                unpack_side(dst, first + p, both[8 * at:8 * at + 8])

    def ends(sends, recvs, d, m):
        (s_row, s_col, s_cor), (r_row, r_col, r_cor) = sends, recvs
        if d in (FROM_UP, FROM_DOWN):
            return s_row.at[d], r_row.at[m]
        if d == FROM_SIDE:
            return s_col, r_col
        return s_cor.at[d - FROM_DUP], r_cor.at[m - FROM_DUP]

    def remote(kind, b, j, d, m, src, dst):
        r, c = peers[d]
        return pltpu.make_async_remote_copy(
            src_ref=src, dst_ref=dst, send_sem=ssem.at[kind + j, d], recv_sem=rsem.at[b, kind + j, m],
            device_id=(grp, c, r), device_id_type=MESH)

    send_bufs = ((sx_row, sx_col, sx_cor), (sh_row, sh_col, sh_cor), (sc_row, sc_col, sc_cor))
    recv_bufs = ((rx_row, rx_col, rx_cor), (rh_row, rh_col, rh_cor), (rc_row, rc_col, rc_cor))

    def frame_ends(b, j, d, m):
        sends, recvs = ([x.at[b, j] for x in bufs[FRAME]] for bufs in (send_bufs, recv_bufs))
        src, dst = ends(sends, recvs, d, m)
        if j and d < FROM_SIDE:
            src, dst = src.at[pl.ds(0, 1)], dst.at[pl.ds(0, 1)]
        if j and d == FROM_SIDE:
            src, dst = src.at[pl.ds(0, 4)], dst.at[pl.ds(0, 4)]
        return src, dst

    def frame_out(b, j, d):
        remote(FRAME, b, 3 + j, d, MIRROR[d], *frame_ends(b, j, d, MIRROR[d])).start()

    def frame_in(b, j, d):
        remote(FRAME, b, 3 + j, d, d, *frame_ends(b, j, d, d)).wait_recv()

    def send_state(kind, b, d, half=None):
        sends, recvs = ([x.at[b] for x in bufs[kind]] for bufs in (send_bufs, recv_bufs))
        src, dst = ends(sends, recvs, d, MIRROR[d])
        if half is not None:
            src, dst = src.at[pl.ds(4 * half, 4)], dst.at[pl.ds(4 * half, 4)]
        remote(kind, b, 0, d, MIRROR[d], src, dst).start()

    def state_in(b, d):
        for kind in (HID, CELL):
            sends, recvs = ([x.at[b] for x in bufs[kind]] for bufs in (send_bufs, recv_bufs))
            src, dst = ends(sends, recvs, d, d)
            remote(kind, b, 0, d, d, src, dst).wait_recv()

    def drain(d):
        which = 0 if d < FROM_SIDE else 1 if d == FROM_SIDE else 2
        for kind in (HID, CELL):
            at = (slice(None),) + (() if d == FROM_SIDE else (d if d < FROM_SIDE else d - FROM_DUP,))
            remote(kind, 0, 0, d, d, send_bufs[kind][which].at[at], recv_bufs[kind][which].at[at]).wait_send()
        for j in range(DEPTH):
            frame_in(BLOCKS, j, d)
            if d == FROM_SIDE:
                at = (slice(None), j) + ((pl.ds(0, 4),) if j else ())
            elif d < FROM_SIDE:
                at = (slice(None), j, d) + ((pl.ds(0, 1),) if j else ())
            else:
                at = (slice(None), j, d - FROM_DUP)
            remote(FRAME, 0, 3 + j, d, d, send_bufs[FRAME][which].at[at], recv_bufs[FRAME][which].at[at]).wait_send()

    def send_state_cols(b, part):
        pack_cols(hs, sh_col.at[b], sh_cor.at[b], part)
        for at, i in list(enumerate(COL_ORDER))[4 * part:4 * part + 4]:
            for u in range(2):
                sc_col[b, at, 4 * u:4 * u + 4] = cs[1 + 2 * i + u, pl.ds(cstrip_from, 4), :]
        for kind in (HID, CELL):
            send_state(kind, b, FROM_SIDE, part)

    def send_state_rest(b):
        pack_rows(hs, sh_row.at[b])
        sc_row[b, 0] = cs[1, 0:OWN, :]
        sc_row[b, 1] = cs[PAIRS, 0:OWN, :]
        sc_cor[b, 0] = cs[1, pl.ds(cstrip_at, 8), :]
        sc_cor[b, 1] = cs[PAIRS, pl.ds(cstrip_at, 8), :]

        def out(d):
            if d != FROM_SIDE:
                for kind in (HID, CELL):
                    send_state(kind, b, d)

        toward(out)

    def receive_state(b):
        toward(lambda d: state_in(b, d))
        unpack_bf16(hs, lambda w, p: rh_row[b, w, p], lambda i: rh_col[b, i], lambda w: rh_cor[b, w])
        for at, i in enumerate(COL_ORDER):
            for u in range(2):
                cs[1 + 2 * i + u, pl.ds(cstrip_to, 4), :] = rc_col[b, at, 4 * u:4 * u + 4]
        for which, at, there in ((0, 0, has_up), (1, 1 + PAIRS, has_down)):
            cs[at, 0:OWN, :] = jnp.where(there, rc_row[b, which], 0.0)
            cs[at, 64:72, :] = jnp.where(there, rc_cor[b, which], 0.0)

    def take_frame(b, j, pairs):
        for q in pairs:
            for s in range(2):
                both = jnp.concatenate([fbuf[j, s, 2 * q], fbuf[j, s, 2 * q + 1]], axis=1).astype(F32)
                xs[j, EDGE + q, pl.ds(8 + s, 32, stride=2), :] = both
            wrap_first(xs.at[j], EDGE + q)

    def pack_frame(b, j):
        if j:
            pack_narrow(xs.at[j], sx_row.at[b, j], sx_col.at[b, j], sx_cor.at[b, j])
            return
        pack_rows(xs.at[j], sx_row.at[b, j])
        for part in range(2):
            pack_cols(xs.at[j], sx_col.at[b, j], sx_cor.at[b, j], part)

    def tasks(j):
        first, count, width = region(j)
        if count == 18:
            lists = ((1, 2, 3, 16, 17, 18), (4, 5, 6, 13, 14, 15), (7, 8, 9, 10, 11, 12))
        else:
            lists = ((2, 3, 4, 5, 14, 15, 16, 17), (6, 7, 8, 9, 10, 11, 12, 13))
        out, base = [], 0
        for pairs in lists:
            out.append((j, pairs, width, base))
            base += len(pairs) * width
        return out

    def product(src, task, w):
        _, pairs, width, _ = task
        low = (lane < 64)[0:width]
        total = None
        for dx in range(3):
            at = pl.ds(6 + 2 * dx, width)
            r = {q: src[q, at, :] for q in sorted({p + e for p in pairs for e in (-1, 0, 1)})}
            own = jnp.concatenate([r[q] for q in pairs], axis=0).astype(BF16)
            near = jnp.concatenate([jnp.where(low, r[q + 1], r[q - 1]) for q in pairs], axis=0).astype(BF16)
            part = jnp.dot(jnp.concatenate([own, near], axis=1), w[dx * 256:dx * 256 + 256, :], preferred_element_type=F32)
            total = part if total is None else total + part
        return total

    def unpack_frame(b, j):
        if j:
            unpack_narrow(xs.at[j], lambda w: rx_row[b, j, w, 0], lambda i: rx_col[b, j, i], lambda w: rx_cor[b, j, w])
            return
        unpack_bf16(xs.at[j], lambda w, p: rx_row[b, j, w, p], lambda i: rx_col[b, j, i], lambda w: rx_cor[b, j, w])

    def x_gates(src, slot, task):
        j, pairs, width, at = task
        xg[j, at:at + len(pairs) * width, :] = product(src, task, wx) + bias[...]

    all_tasks = [t for j in range(DEPTH) for t in tasks(j)]
    last_of_step = [i + 1 == len(all_tasks) or all_tasks[i + 1][0] != t[0] for i, t in enumerate(all_tasks)]

    def frames_wait(following):
        for j in range(DEPTH):
            frame_copy(0, j).wait()

    def fetch(b):
        for j in range(DEPTH):
            frame_copy(b * DEPTH + j, j).start()

    def h_gates(src, slot, task):
        j, pairs, width, base = task
        rows = len(pairs) * width
        gts[slot, 0:rows, :] = product(src, task, wh) + xg[j, base:base + rows, :]

    def cells(slot, task, t):
        j, pairs, width, _ = task
        for q, at in enumerate(pairs):
            rows_q = pl.ds(q * width, width)
            gi, gf, go, gg = (gts[slot, rows_q, 128 * i:128 * i + 128] for i in range(4))
            c_old = cs[at - 1, 0:width, :]
            ti, tf, to = jnp.tanh(0.5 * gi), jnp.tanh(0.5 * gf), jnp.tanh(0.5 * go)
            c_new = 0.5 * ((tf + 1.0) * c_old + (ti + 1.0) * jnp.tanh(gg))
            cs[at - 1, 0:width, :] = c_new
            h_new = 0.5 * (to + 1.0) * jnp.tanh(c_new)
            if at < EDGE:
                h_new = h_new * up_mask
            if at >= EDGE + PAIRS:
                h_new = h_new * down_mask
            hs[at, 8:72, :] = h_new[0:OWN]
            hs[at, 80:88, :] = h_new[0:8]
            if width == 72:
                unpack_side(hs, at, h_new[64:72])
            if EDGE <= at < EDGE + PAIRS:
                for s in range(2):
                    both = hs[at, pl.ds(8 + s, 32, stride=2), :].astype(BF16)
                    h_out[t, s, 2 * (at - EDGE)] = both[:, 0:64]
                    h_out[t, s, 2 * (at - EDGE) + 1] = both[:, 64:128]

    def run(hid_block, x_block):
        todo = []
        if hid_block is not None:
            todo += [(hs, t, True) for t in all_tasks]
        if x_block is not None:
            todo += [(xs.at[t[0]], t, False) for t in all_tasks]
        def ahead(i):
            src, task, hidden = todo[i]
            (h_gates if hidden else x_gates)(src, i % 2, task)

        ahead(0)
        for i, (src, task, hidden) in enumerate(todo):
            n = i % len(all_tasks)
            if hidden and x_block is not None and n + 1 == len(all_tasks):
                for j in range(DEPTH):
                    unpack_frame(x_block, j)
            if i + 1 < len(todo):
                ahead(i + 1)
            if hidden:
                cells(i % 2, task, hid_block * DEPTH + task[0])
                if x_block is not None and n + 2 == len(all_tasks):
                    send_state_cols(hid_block + 1, 0)
                    send_state_rest(hid_block + 1)
                    toward(lambda d: [frame_in(x_block, j, d) for j in range(DEPTH)])
                if x_block is not None and n + 1 == len(all_tasks):
                    send_state_cols(hid_block + 1, 1)
            elif last_of_step[n]:
                take_frame(x_block + 1, task[0], range(PAIRS))
                pack_frame(x_block + 1, task[0])
                if task[0] == 1:
                    toward(lambda d: [frame_out(x_block + 1, j, d) for j in (0, 1)])
                if task[0] == 2:
                    toward(lambda d: frame_out(x_block + 1, 2, d))

    def weights(src, dst):
        zero = jnp.zeros((64, 64), BF16)
        for dx in range(3):
            for k, q in enumerate((0, 1, 2, -1)):
                for g in range(4):
                    parts = []
                    for p in range(2):
                        dy = q - p + 1
                        parts.append(src[dy, dx, :, 64 * g:64 * g + 64] if 0 <= dy <= 2 else zero)
                    dst[dx * 256 + k * 64:dx * 256 + k * 64 + 64, 128 * g:128 * g + 128] = jnp.concatenate(parts, axis=1)

    for j in range(DEPTH):
        frame_copy(0, j).wait()
        take_frame(0, j, range(PAIRS))
        pack_frame(0, j)
        if j == 0:
            pl.semaphore_wait(barrier, 3 + 2 * (has_up & has_down).astype(jnp.int32))
        toward(lambda d: frame_out(0, j, d))
    for j in range(DEPTH):
        frame_copy(DEPTH + j, j).start()
    for cp in inputs:
        cp.wait()
    ingest(lambda s, r: h_in[s, r], hs.at[pl.ds(EDGE, PAIRS), pl.ds(8, OWN)])
    ingest(lambda s, r: c_in[s, r], cs.at[pl.ds(1, PAIRS), pl.ds(0, OWN)])
    for q in range(PAIRS):
        wrap_first(hs, EDGE + q)
    for part in range(2):
        send_state_cols(0, part)
    send_state_rest(0)
    weights(wx_in, wx)
    weights(wh_in, wh)
    for g in range(4):
        piece = bias_in[:, 64 * g:64 * g + 64]
        bias[:, 128 * g:128 * g + 128] = jnp.concatenate([piece, piece], axis=1)
    for j in range(DEPTH):
        toward(lambda d: frame_in(0, j, d))
        unpack_frame(0, j)
        if j == DEPTH - 1:
            frames_wait(1)
        for task in tasks(j):
            x_gates(xs.at[j], 0, task)
    for j in range(DEPTH):
        take_frame(1, j, range(PAIRS))
        pack_frame(1, j)
    toward(lambda d: [frame_out(1, j, d) for j in range(DEPTH)])
    fetch(2)

    def block(b, _):
        pl.when(b + 2 < BLOCKS)(lambda: frames_wait(b + 2))
        receive_state(b)
        run(b, b + 1)
        pl.when(b + 3 < BLOCKS)(lambda: fetch(b + 3))
        return 0

    lax.fori_loop(0, BLOCKS - 1, block, 0)
    receive_state(BLOCKS - 1)
    run(BLOCKS - 1, None)

    for q in range(PAIRS):
        for s in range(2):
            both = cs[1 + q, pl.ds(s, 32, stride=2), :]
            c_out[s, 2 * q] = both[:, 0:64]
            c_out[s, 2 * q + 1] = both[:, 64:128]

    toward(drain)


def write_out(h, c, h_out, c_out, sem):
    copies = [pltpu.make_async_copy(h.at[t], h_out.at[t], sem.at[t]) for t in range(STEPS)]
    copies.append(pltpu.make_async_copy(c, c_out, sem.at[STEPS]))
    for cp in copies:
        cp.start()
    for cp in copies:
        cp.wait()


def solution(mesh):
    frame_spec = P(None, "batch", "rows", "cols", None)
    state_spec = P("batch", "rows", "cols", None)

    def local_run(frames, w_x, w_h, gate_bias, h_init, c_init):
        vmem = pl.BlockSpec(memory_space=pltpu.VMEM)
        hbm = pl.BlockSpec(memory_space=pltpu.HBM)
        most = max(region(j)[1] * region(j)[2] for j in range(DEPTH))
        strips = [
            [(BLOCKS, DEPTH, 2, HP, OWN, 128), (BLOCKS, DEPTH, 8, 16, 128), (BLOCKS, DEPTH, 2, 16, 128)],
            [(BLOCKS, 2, HP, OWN, 128), (BLOCKS, 8, 16, 128), (BLOCKS, 2, 16, 128)],
            [(BLOCKS, 2, OWN, 128), (BLOCKS, PAIRS // 2, 8, 128), (BLOCKS, 2, 8, 128)],
        ]
        strips[0] = [(s[0] + 1,) + s[1:] for s in strips[0]]
        strip_bufs = [pltpu.VMEM(s, BF16 if k < 2 else F32) for k in range(3) for s in strips[k]]
        h_pairs, c_pairs = pl.pallas_call(
            kernel,
            out_shape=(pltpu.VMEM(frames.shape, BF16), pltpu.VMEM(c_init.shape, F32)),
            in_specs=[hbm] * 6,
            out_specs=(vmem, vmem),
            scratch_shapes=[
                pltpu.VMEM((DEPTH,) + h_init.shape, BF16),
                pltpu.VMEM(w_x.shape, BF16),
                pltpu.VMEM(w_h.shape, BF16),
                pltpu.VMEM((1, 256), F32),
                pltpu.VMEM(h_init.shape, BF16),
                pltpu.VMEM(c_init.shape, F32),
                pltpu.VMEM((DEPTH, ROWS_ALL, SUBL, 128), F32),
                pltpu.VMEM((ROWS_ALL, SUBL, 128), F32),
                pltpu.VMEM((PAIRS + 2, 72, 128), F32),
                pltpu.VMEM((DEPTH, most, 512), F32),
                pltpu.VMEM((2, 512, 512), F32),
                pltpu.VMEM((768, 512), BF16),
                pltpu.VMEM((768, 512), BF16),
                pltpu.VMEM((1, 512), F32),
                *strip_bufs, *strip_bufs,
                pltpu.SemaphoreType.DMA((DEPTH,)),
                pltpu.SemaphoreType.DMA((5,)),
                pltpu.SemaphoreType.DMA((3 + DEPTH, 5)),
                pltpu.SemaphoreType.DMA((BLOCKS + 1, 3 + DEPTH, 5)),
            ],
            compiler_params=pltpu.CompilerParams(collective_id=0, has_side_effects=True, vmem_limit_bytes=56 * 2**20),
        )(frames, w_x, w_h, gate_bias.reshape(1, 256), h_init, c_init)
        return pl.pallas_call(
            write_out,
            out_shape=(jax.ShapeDtypeStruct(frames.shape, BF16), jax.ShapeDtypeStruct(c_init.shape, F32)),
            in_specs=[vmem, vmem],
            out_specs=(hbm, hbm),
            scratch_shapes=[pltpu.SemaphoreType.DMA((STEPS + 1,))],
            compiler_params=pltpu.CompilerParams(vmem_limit_bytes=16 * 2**20),
        )(h_pairs, c_pairs)

    return jax.shard_map(local_run, mesh=mesh, in_specs=(frame_spec, P(), P(), P(), state_spec, state_spec),
                         out_specs=(frame_spec, state_spec), check_vma=False)
```

```python
import functools

import jax
import jax.numpy as jnp
from jax import lax
from jax.experimental import pallas as pl
from jax.experimental.pallas import tpu as pltpu
from jax.sharding import PartitionSpec as P

MESH = pl.DeviceIdType.MESH
F32, BF16 = jnp.float32, jnp.bfloat16

DEPTH = 3
STEPS = 12
BLOCKS = STEPS // DEPTH
PAIRS = 16
OWN = 64
EDGE = 2
HP = -(-DEPTH // 2)
ROWS_ALL = PAIRS + 2 * EDGE
SUBL = 88
FROM_UP, FROM_DOWN, FROM_SIDE, FROM_DUP, FROM_DDOWN = DIRS = range(5)
MIRROR = (FROM_DOWN, FROM_UP, FROM_SIDE, FROM_DDOWN, FROM_DUP)
FRAME, HID, CELL = range(3)
MID, HALO = slice(8, 72), slice(72, 80)
BEFORE, AFTER = slice(0, 8), slice(80, 88)
FIRST, COWN, CHALO = slice(8, 16), slice(0, 64), slice(64, 72)
LEFT, RIGHT = slice(0, 64), slice(64, 128)
COL_ORDER = (0, 1, 6, 7, 2, 3, 4, 5)


def region(j):
    halo = DEPTH - 1 - j
    extra = -(-halo // 2)
    return EDGE - extra, PAIRS + 2 * extra, 72 if halo else OWN


def kernel(frames, wx_hbm, wh_hbm, bias_hbm, h_hbm, c_hbm, h_out, c_out,
           fbuf, wx_in, wh_in, bias_in, h_in, c_in, xs, hs, cs, xg, gts, wx, wh, bias,
           sx_row, sx_col, sx_cor, sh_row, sh_col, sh_cor, sc_row, sc_col, sc_cor,
           rx_row, rx_col, rx_cor, rh_row, rh_col, rh_cor, rc_row, rc_col, rc_cor,
           fsem, isem, ssem, rsem):
    row, col, grp = lax.axis_index("rows"), lax.axis_index("cols"), lax.axis_index("batch")
    n_rows = lax.axis_size("rows")
    side = 1 - col
    has_up, has_down = row > 0, row < n_rows - 1
    above, below = lax.rem(row + n_rows - 1, n_rows), lax.rem(row + 1, n_rows)
    peers = ((above, col), (below, col), (row, side), (above, side), (below, side))

    lane = lax.broadcasted_iota(jnp.int32, (72, 128), 1)
    subl = lax.broadcasted_iota(jnp.int32, (8, 128), 0)
    col_mask = jnp.where((subl + 2 * (1 - col) >= 2) & (subl < 6 + 2 * col), 1.0, 0.0).astype(F32)
    up_mask = jnp.where(has_up, 1.0, 0.0).astype(F32)
    down_mask = jnp.where(has_down, 1.0, 0.0).astype(F32)

    def frame_copy(t, slot):
        return pltpu.make_async_copy(frames.at[t], fbuf.at[slot], fsem.at[slot])

    for j in range(DEPTH):
        frame_copy(j, j).start()

    inputs = [pltpu.make_async_copy(src, dst, isem.at[i]) for i, (src, dst) in enumerate(
        ((h_hbm, h_in), (c_hbm, c_in), (wx_hbm, wx_in), (wh_hbm, wh_in), (bias_hbm, bias_in)))]
    for cp in inputs:
        cp.start()

    barrier = pltpu.get_barrier_semaphore()
    def toward(fn):
        def both(a, b):
            fn(a)
            fn(b)

        fn(FROM_SIDE)
        pl.when(has_up)(lambda: both(FROM_UP, FROM_DUP))
        pl.when(has_down)(lambda: both(FROM_DOWN, FROM_DDOWN))

    toward(lambda d: pl.semaphore_signal(barrier, inc=1, device_id=(grp, peers[d][1], peers[d][0]), device_id_type=MESH))

    def ingest(load, dst):
        def body(i, _):
            for u in range(4):
                q = i * 4 + u
                for s in range(2):
                    both = jnp.concatenate([load(s, 2 * q), load(s, 2 * q + 1)], axis=1).astype(F32)
                    dst[q, pl.ds(s, 32, stride=2), :] = both
            return 0
        lax.fori_loop(0, PAIRS // 4, body, 0)

    def wrap_first(ref, q):
        ref[q, AFTER, :] = ref[q, FIRST, :]

    nil = jnp.zeros((SUBL, 128), F32)
    for q in (0, 1, ROWS_ALL - 2, ROWS_ALL - 1):
        hs[q] = nil
        for j in range(2 * DEPTH):
            xs[j, q] = nil
    for q in (0, PAIRS + 1):
        cs[q] = nil[0:72]
    for q in range(PAIRS):
        cs[1 + q, CHALO, :] = nil[BEFORE]
        for j in (1, 2, 4, 5):
            xs[j, EDGE + q, BEFORE, :] = nil[BEFORE]
            xs[j, EDGE + q, HALO, :] = nil[BEFORE]

    strip_at = pl.multiple_of(8 + 56 * (1 - col), 8)
    cstrip_at = pl.multiple_of(56 * (1 - col), 8)
    cstrip_from = pl.multiple_of(60 * (1 - col), 4)
    cstrip_to = pl.multiple_of(64 + 4 * col, 4)

    def pack_rows(src, s_row):
        for p in range(HP):
            s_row[0, p] = src[EDGE + p, MID, :].astype(BF16)
            s_row[1, p] = src[EDGE + PAIRS - HP + p, MID, :].astype(BF16)

    def pack_cols(src, s_col, s_cor, part):
        for at, i in list(enumerate(COL_ORDER))[4 * part:4 * part + 4]:
            two = jnp.concatenate([src[EDGE + 2 * i, pl.ds(strip_at, 8), :],
                                   src[EDGE + 2 * i + 1, pl.ds(strip_at, 8), :]], axis=0).astype(BF16)
            s_col[at] = two
            if i == 0:
                s_cor[0] = two
            if i == PAIRS // 2 - 1:
                s_cor[1] = two

    def pack_narrow(src, s_row, s_col, s_cor):
        s_row[0, 0] = src[EDGE, MID, :].astype(BF16)
        s_row[1, 0] = src[EDGE + PAIRS - 1, MID, :].astype(BF16)
        for i in range(PAIRS // 4):
            s_col[i] = jnp.concatenate([src[EDGE + 4 * i + u, pl.ds(8 + cstrip_from, 4), :] for u in range(4)],
                                       axis=0).astype(BF16)
        for side_of, at in ((0, EDGE), (1, EDGE + PAIRS - 1)):
            edge = src[at, pl.ds(strip_at, 8), :]
            s_cor[side_of] = jnp.concatenate([edge, edge], axis=0).astype(BF16)

    def unpack_narrow(dst, get_row, get_col, get_cor):
        for i in range(PAIRS // 4):
            four = get_col(i).astype(F32)
            for u in range(4):
                strip = four[4 * u:4 * u + 4]
                dst[EDGE + 4 * i + u, pl.ds(8 + cstrip_to, 4), :] = strip
                dst[EDGE + 4 * i + u, pl.ds(cstrip_to - 64, 4), :] = strip
        for which, at, there in ((0, EDGE - 1, has_up), (1, EDGE + PAIRS, has_down)):
            strip = jnp.where(there, get_row(which).astype(F32), 0.0)
            dst[at, MID, :] = strip
            dst[at, AFTER, :] = strip[BEFORE]
            unpack_side(dst, at, jnp.where(there, get_cor(which).astype(F32)[BEFORE], 0.0))

    def unpack_side(dst, q, strip):
        strip = strip * col_mask
        dst[q, HALO, :] = strip
        dst[q, BEFORE, :] = strip

    def unpack_bf16(dst, get_row, get_col, get_cor):
        for at, i in enumerate(COL_ORDER):
            both = get_col(at).astype(F32)
            unpack_side(dst, EDGE + 2 * i, both[BEFORE])
            unpack_side(dst, EDGE + 2 * i + 1, both[8:16])

        for which, first, there in ((0, EDGE - HP, has_up), (1, EDGE + PAIRS, has_down)):
            both = jnp.where(there, get_cor(which).astype(F32), 0.0)
            for p in range(HP):
                strip = jnp.where(there, get_row(which, p).astype(F32), 0.0)
                dst[first + p, MID, :] = strip
                dst[first + p, AFTER, :] = strip[BEFORE]
                at = 2 - HP + p if which == 0 else p
                unpack_side(dst, first + p, both[8 * at:8 * at + 8])

    def ends(sends, recvs, d, m):
        (s_row, s_col, s_cor), (r_row, r_col, r_cor) = sends, recvs
        if d in (FROM_UP, FROM_DOWN):
            return s_row.at[d], r_row.at[m]
        if d == FROM_SIDE:
            return s_col, r_col
        return s_cor.at[d - FROM_DUP], r_cor.at[m - FROM_DUP]

    def remote(kind, b, j, d, m, src, dst):
        r, c = peers[d]
        return pltpu.make_async_remote_copy(
            src_ref=src, dst_ref=dst, send_sem=ssem.at[kind + j, d], recv_sem=rsem.at[b, kind + j, m],
            device_id=(grp, c, r), device_id_type=MESH)

    send_bufs = ((sx_row, sx_col, sx_cor), (sh_row, sh_col, sh_cor), (sc_row, sc_col, sc_cor))
    recv_bufs = ((rx_row, rx_col, rx_cor), (rh_row, rh_col, rh_cor), (rc_row, rc_col, rc_cor))

    def frame_ends(b, j, d, m):
        sends, recvs = ([x.at[b, j] for x in bufs[FRAME]] for bufs in (send_bufs, recv_bufs))
        src, dst = ends(sends, recvs, d, m)
        if j and d < FROM_SIDE:
            src, dst = src.at[pl.ds(0, 1)], dst.at[pl.ds(0, 1)]
        if j and d == FROM_SIDE:
            src, dst = src.at[pl.ds(0, 4)], dst.at[pl.ds(0, 4)]
        return src, dst

    def frame_out(b, j, d):
        remote(FRAME, b, 3 + j, d, MIRROR[d], *frame_ends(b, j, d, MIRROR[d])).start()

    def frame_in(b, j, d):
        remote(FRAME, b, 3 + j, d, d, *frame_ends(b, j, d, d)).wait_recv()

    def send_state(kind, b, d, half=None):
        sends, recvs = ([x.at[b] for x in bufs[kind]] for bufs in (send_bufs, recv_bufs))
        src, dst = ends(sends, recvs, d, MIRROR[d])
        if half is not None:
            src, dst = src.at[pl.ds(4 * half, 4)], dst.at[pl.ds(4 * half, 4)]
        remote(kind, b, 0, d, MIRROR[d], src, dst).start()

    def state_in(b, d):
        for kind in (HID, CELL):
            sends, recvs = ([x.at[b] for x in bufs[kind]] for bufs in (send_bufs, recv_bufs))
            src, dst = ends(sends, recvs, d, d)
            remote(kind, b, 0, d, d, src, dst).wait_recv()

    def drain(d):
        which = 0 if d < FROM_SIDE else 1 if d == FROM_SIDE else 2
        for kind in (HID, CELL):
            at = (slice(None),) + (() if d == FROM_SIDE else (d if d < FROM_SIDE else d - FROM_DUP,))
            remote(kind, 0, 0, d, d, send_bufs[kind][which].at[at], recv_bufs[kind][which].at[at]).wait_send()
        for j in range(DEPTH):
            frame_in(BLOCKS, j, d)
            if d == FROM_SIDE:
                at = (slice(None), j) + ((pl.ds(0, 4),) if j else ())
            elif d < FROM_SIDE:
                at = (slice(None), j, d) + ((pl.ds(0, 1),) if j else ())
            else:
                at = (slice(None), j, d - FROM_DUP)
            remote(FRAME, 0, 3 + j, d, d, send_bufs[FRAME][which].at[at], recv_bufs[FRAME][which].at[at]).wait_send()

    def send_state_cols(b, part):
        pack_cols(hs, sh_col.at[b], sh_cor.at[b], part)
        for at, i in list(enumerate(COL_ORDER))[4 * part:4 * part + 4]:
            for u in range(2):
                sc_col[b, at, 4 * u:4 * u + 4] = cs[1 + 2 * i + u, pl.ds(cstrip_from, 4), :]
        for kind in (HID, CELL):
            send_state(kind, b, FROM_SIDE, part)

    def send_state_rest(b):
        pack_rows(hs, sh_row.at[b])
        sc_row[b, 0] = cs[1, COWN, :]
        sc_row[b, 1] = cs[PAIRS, COWN, :]
        sc_cor[b, 0] = cs[1, pl.ds(cstrip_at, 8), :]
        sc_cor[b, 1] = cs[PAIRS, pl.ds(cstrip_at, 8), :]

        def out(d):
            if d != FROM_SIDE:
                for kind in (HID, CELL):
                    send_state(kind, b, d)

        toward(out)

    def receive_state(b):
        toward(lambda d: state_in(b, d))
        unpack_bf16(hs, lambda w, p: rh_row[b, w, p], lambda i: rh_col[b, i], lambda w: rh_cor[b, w])
        for at, i in enumerate(COL_ORDER):
            for u in range(2):
                cs[1 + 2 * i + u, pl.ds(cstrip_to, 4), :] = rc_col[b, at, 4 * u:4 * u + 4]
        for which, at, there in ((0, 0, has_up), (1, 1 + PAIRS, has_down)):
            cs[at, COWN, :] = jnp.where(there, rc_row[b, which], 0.0)
            cs[at, CHALO, :] = jnp.where(there, rc_cor[b, which], 0.0)

    def plane(b, j):
        return xs.at[lax.rem(b, 2) * DEPTH + j]

    def take_frame(b, j):
        dst = plane(b, j)
        for q in range(PAIRS):
            for s in range(2):
                both = jnp.concatenate([fbuf[j, s, 2 * q], fbuf[j, s, 2 * q + 1]], axis=1).astype(F32)
                dst[EDGE + q, pl.ds(8 + s, 32, stride=2), :] = both
            wrap_first(dst, EDGE + q)
        pack_frame(b, j)

    def pack_frame(b, j):
        if j:
            pack_narrow(plane(b, j), sx_row.at[b, j], sx_col.at[b, j], sx_cor.at[b, j])
            return
        pack_rows(plane(b, j), sx_row.at[b, j])
        for part in range(2):
            pack_cols(plane(b, j), sx_col.at[b, j], sx_cor.at[b, j], part)

    def tasks(j):
        first, count, width = region(j)
        if count == 18:
            lists = ((1, 2, 3, 16, 17, 18), (4, 5, 6, 13, 14, 15), (7, 8, 9, 10, 11, 12))
        else:
            lists = ((2, 3, 4, 5, 14, 15, 16, 17), (6, 7, 8, 9, 10, 11, 12, 13))
        out, base = [], 0
        for pairs in lists:
            out.append((j, pairs, width, base))
            base += len(pairs) * width
        return out

    def product(src, task, w):
        _, pairs, width, _ = task
        low = (lane < 64)[0:width]
        total = None
        for dx in range(3):
            at = pl.ds(6 + 2 * dx, width)
            r = {q: src[q, at, :] for q in sorted({p + e for p in pairs for e in (-1, 0, 1)})}
            own = jnp.concatenate([r[q] for q in pairs], axis=0).astype(BF16)
            near = jnp.concatenate([jnp.where(low, r[q + 1], r[q - 1]) for q in pairs], axis=0).astype(BF16)
            part = jnp.dot(jnp.concatenate([own, near], axis=1), w[dx * 256:dx * 256 + 256, :], preferred_element_type=F32)
            total = part if total is None else total + part
        return total

    def unpack_frame(b, j):
        if j:
            unpack_narrow(plane(b, j), lambda w: rx_row[b, j, w, 0], lambda i: rx_col[b, j, i], lambda w: rx_cor[b, j, w])
            return
        unpack_bf16(plane(b, j), lambda w, p: rx_row[b, j, w, p], lambda i: rx_col[b, j, i], lambda w: rx_cor[b, j, w])

    def x_gates(src, slot, task):
        j, pairs, width, at = task
        xg[j, at:at + len(pairs) * width, :] = product(src, task, wx) + bias[...]

    all_tasks = [t for j in range(DEPTH) for t in tasks(j)]
    def frames_wait():
        for j in range(DEPTH):
            frame_copy(0, j).wait()

    def fetch(b):
        for j in range(DEPTH):
            frame_copy(b * DEPTH + j, j).start()

    def h_gates(src, slot, task):
        j, pairs, width, base = task
        rows = len(pairs) * width
        gts[slot, 0:rows, :] = product(src, task, wh) + xg[j, base:base + rows, :]

    def cells(slot, task, t):
        j, pairs, width, _ = task
        for q, at in enumerate(pairs):
            rows_q = pl.ds(q * width, width)
            gi, gf, go, gg = (gts[slot, rows_q, 128 * i:128 * i + 128] for i in range(4))
            c_old = cs[at - 1, 0:width, :]
            ti, tf, to = jnp.tanh(0.5 * gi), jnp.tanh(0.5 * gf), jnp.tanh(0.5 * go)
            c_new = 0.5 * ((tf + 1.0) * c_old + (ti + 1.0) * jnp.tanh(gg))
            cs[at - 1, 0:width, :] = c_new
            h_new = 0.5 * (to + 1.0) * jnp.tanh(c_new)
            if at < EDGE:
                h_new = h_new * up_mask
            if at >= EDGE + PAIRS:
                h_new = h_new * down_mask
            hs[at, MID, :] = h_new[0:OWN]
            hs[at, AFTER, :] = h_new[BEFORE]
            if width == 72:
                unpack_side(hs, at, h_new[64:72])
            if EDGE <= at < EDGE + PAIRS:
                for s in range(2):
                    both = hs[at, pl.ds(8 + s, 32, stride=2), :].astype(BF16)
                    h_out[t, s, 2 * (at - EDGE)] = both[:, LEFT]
                    h_out[t, s, 2 * (at - EDGE) + 1] = both[:, RIGHT]

    def run(hid_block, x_block):
        todo = []
        if hid_block is not None:
            todo += [(hs, t, True) for t in all_tasks]
        if x_block is not None:
            todo += [(plane(x_block, t[0]), t, False) for t in all_tasks]
        def ahead(i):
            src, task, hidden = todo[i]
            (h_gates if hidden else x_gates)(src, i % 2, task)

        ahead(0)
        for i, (src, task, hidden) in enumerate(todo):
            n = i % len(all_tasks)
            if hidden and x_block is not None and n + 1 == len(all_tasks):
                for j in range(DEPTH):
                    unpack_frame(x_block, j)
            if i + 1 < len(todo):
                ahead(i + 1)
            if hidden:
                cells(i % 2, task, hid_block * DEPTH + task[0])
                if x_block is None:
                    continue
                if n < DEPTH:
                    take_frame(x_block + 1, n)
                if n + 2 == len(all_tasks):
                    send_state_cols(hid_block + 1, 0)
                    send_state_rest(hid_block + 1)
                    toward(lambda d: [frame_in(x_block, j, d) for j in range(DEPTH)])
                if n + 1 == len(all_tasks):
                    send_state_cols(hid_block + 1, 1)
                    toward(lambda d: [frame_out(x_block + 1, j, d) for j in range(DEPTH)])

    def weights(src, dst):
        zero = jnp.zeros((64, 64), BF16)
        for dx in range(3):
            for k, q in enumerate((0, 1, 2, -1)):
                for g in range(4):
                    parts = []
                    for p in range(2):
                        dy = q - p + 1
                        parts.append(src[dy, dx, :, 64 * g:64 * g + 64] if 0 <= dy <= 2 else zero)
                    dst[dx * 256 + k * 64:dx * 256 + k * 64 + 64, 128 * g:128 * g + 128] = jnp.concatenate(parts, axis=1)

    for j in range(DEPTH):
        frame_copy(0, j).wait()
        take_frame(0, j)
        if j == 0:
            pl.semaphore_wait(barrier, 3 + 2 * (has_up & has_down).astype(jnp.int32))
        toward(lambda d: frame_out(0, j, d))
    for j in range(DEPTH):
        frame_copy(DEPTH + j, j).start()
    for cp in inputs:
        cp.wait()
    ingest(lambda s, r: h_in[s, r], hs.at[pl.ds(EDGE, PAIRS), pl.ds(8, OWN)])
    ingest(lambda s, r: c_in[s, r], cs.at[pl.ds(1, PAIRS), pl.ds(0, OWN)])
    for q in range(PAIRS):
        wrap_first(hs, EDGE + q)
    for part in range(2):
        send_state_cols(0, part)
    send_state_rest(0)
    weights(wx_in, wx)
    weights(wh_in, wh)
    for g in range(4):
        piece = bias_in[:, 64 * g:64 * g + 64]
        bias[:, 128 * g:128 * g + 128] = jnp.concatenate([piece, piece], axis=1)
    frames_wait()
    for j in range(DEPTH):
        take_frame(1, j)
    toward(lambda d: [frame_out(1, j, d) for j in range(DEPTH)])
    fetch(2)
    for j in range(DEPTH):
        toward(lambda d: frame_in(0, j, d))
        unpack_frame(0, j)
        for task in tasks(j):
            x_gates(plane(0, j), 0, task)

    def block(b, _):
        pl.when(b + 2 < BLOCKS)(frames_wait)
        receive_state(b)
        run(b, b + 1)
        pl.when(b + 3 < BLOCKS)(lambda: fetch(b + 3))
        return 0

    lax.fori_loop(0, BLOCKS - 1, block, 0)
    receive_state(BLOCKS - 1)
    run(BLOCKS - 1, None)

    for q in range(PAIRS):
        for s in range(2):
            both = cs[1 + q, pl.ds(s, 32, stride=2), :]
            c_out[s, 2 * q] = both[:, LEFT]
            c_out[s, 2 * q + 1] = both[:, RIGHT]

    toward(drain)


def write_out(h, c, h_out, c_out, sem):
    copies = [pltpu.make_async_copy(h.at[t], h_out.at[t], sem.at[t]) for t in range(STEPS)]
    copies.append(pltpu.make_async_copy(c, c_out, sem.at[STEPS]))
    for cp in copies:
        cp.start()
    for cp in copies:
        cp.wait()


def solution(mesh):
    frame_spec = P(None, "batch", "rows", "cols", None)
    state_spec = P("batch", "rows", "cols", None)

    def local_run(frames, w_x, w_h, gate_bias, h_init, c_init):
        vmem = pl.BlockSpec(memory_space=pltpu.VMEM)
        hbm = pl.BlockSpec(memory_space=pltpu.HBM)
        most = max(region(j)[1] * region(j)[2] for j in range(DEPTH))
        strips = [
            [(BLOCKS, DEPTH, 2, HP, OWN, 128), (BLOCKS, DEPTH, 8, 16, 128), (BLOCKS, DEPTH, 2, 16, 128)],
            [(BLOCKS, 2, HP, OWN, 128), (BLOCKS, 8, 16, 128), (BLOCKS, 2, 16, 128)],
            [(BLOCKS, 2, OWN, 128), (BLOCKS, PAIRS // 2, 8, 128), (BLOCKS, 2, 8, 128)],
        ]
        strips[0] = [(s[0] + 1,) + s[1:] for s in strips[0]]
        strip_bufs = [pltpu.VMEM(s, BF16 if k < 2 else F32) for k in range(3) for s in strips[k]]
        h_pairs, c_pairs = pl.pallas_call(
            kernel,
            out_shape=(pltpu.VMEM(frames.shape, BF16), pltpu.VMEM(c_init.shape, F32)),
            in_specs=[hbm] * 6,
            out_specs=(vmem, vmem),
            scratch_shapes=[
                pltpu.VMEM((DEPTH,) + h_init.shape, BF16),
                pltpu.VMEM(w_x.shape, BF16),
                pltpu.VMEM(w_h.shape, BF16),
                pltpu.VMEM((1, 256), F32),
                pltpu.VMEM(h_init.shape, BF16),
                pltpu.VMEM(c_init.shape, F32),
                pltpu.VMEM((2 * DEPTH, ROWS_ALL, SUBL, 128), F32),
                pltpu.VMEM((ROWS_ALL, SUBL, 128), F32),
                pltpu.VMEM((PAIRS + 2, 72, 128), F32),
                pltpu.VMEM((DEPTH, most, 512), F32),
                pltpu.VMEM((2, 512, 512), F32),
                pltpu.VMEM((768, 512), BF16),
                pltpu.VMEM((768, 512), BF16),
                pltpu.VMEM((1, 512), F32),
                *strip_bufs, *strip_bufs,
                pltpu.SemaphoreType.DMA((DEPTH,)),
                pltpu.SemaphoreType.DMA((5,)),
                pltpu.SemaphoreType.DMA((3 + DEPTH, 5)),
                pltpu.SemaphoreType.DMA((BLOCKS + 1, 3 + DEPTH, 5)),
            ],
            compiler_params=pltpu.CompilerParams(collective_id=0, has_side_effects=True, vmem_limit_bytes=56 * 2**20),
        )(frames, w_x, w_h, gate_bias.reshape(1, 256), h_init, c_init)
        return pl.pallas_call(
            write_out,
            out_shape=(jax.ShapeDtypeStruct(frames.shape, BF16), jax.ShapeDtypeStruct(c_init.shape, F32)),
            in_specs=[vmem, vmem],
            out_specs=(hbm, hbm),
            scratch_shapes=[pltpu.SemaphoreType.DMA((STEPS + 1,))],
            compiler_params=pltpu.CompilerParams(vmem_limit_bytes=16 * 2**20),
        )(h_pairs, c_pairs)

    return jax.shard_map(local_run, mesh=mesh, in_specs=(frame_spec, P(), P(), P(), state_spec, state_spec),
                         out_specs=(frame_spec, state_spec), check_vma=False)
```

```python
import functools

import jax
import jax.numpy as jnp
from jax import lax
from jax.experimental import pallas as pl
from jax.experimental.pallas import tpu as pltpu
from jax.sharding import PartitionSpec as P

MESH = pl.DeviceIdType.MESH
F32, BF16 = jnp.float32, jnp.bfloat16

DEPTH = 3
STEPS = 12
BLOCKS = STEPS // DEPTH
PAIRS = 16
OWN = 64
EDGE = 2
HP = -(-DEPTH // 2)
ROWS_ALL = PAIRS + 2 * EDGE
SUBL = 88
FROM_UP, FROM_DOWN, FROM_SIDE, FROM_DUP, FROM_DDOWN = DIRS = range(5)
MIRROR = (FROM_DOWN, FROM_UP, FROM_SIDE, FROM_DDOWN, FROM_DUP)
FRAME, HID, CELL = range(3)
MID, HALO = slice(8, 72), slice(72, 80)
BEFORE, AFTER = slice(0, 8), slice(80, 88)
FIRST, COWN, CHALO = slice(8, 16), slice(0, 64), slice(64, 72)
LEFT, RIGHT = slice(0, 64), slice(64, 128)
COL_ORDER = (0, 1, 6, 7, 2, 3, 4, 5)


def region(j):
    halo = DEPTH - 1 - j
    extra = -(-halo // 2)
    return EDGE - extra, PAIRS + 2 * extra, 72 if halo else OWN


def kernel(frames, wx_hbm, wh_hbm, bias_hbm, h_hbm, c_hbm, h_out, c_out,
           fbuf, wx_in, wh_in, bias_in, h_in, c_in, xs, hs, cs, xg, gts, wx, wh, bias,
           sx_row, sx_col, sx_cor, sh_row, sh_col, sh_cor, sc_row, sc_col, sc_cor,
           rx_row, rx_col, rx_cor, rh_row, rh_col, rh_cor, rc_row, rc_col, rc_cor,
           fsem, isem, ssem, rsem):
    row, col, grp = lax.axis_index("rows"), lax.axis_index("cols"), lax.axis_index("batch")
    n_rows = lax.axis_size("rows")
    side = 1 - col
    has_up, has_down = row > 0, row < n_rows - 1
    above, below = lax.rem(row + n_rows - 1, n_rows), lax.rem(row + 1, n_rows)
    peers = ((above, col), (below, col), (row, side), (above, side), (below, side))

    lane = lax.broadcasted_iota(jnp.int32, (72, 128), 1)
    subl = lax.broadcasted_iota(jnp.int32, (8, 128), 0)
    col_mask = jnp.where((subl + 2 * (1 - col) >= 2) & (subl < 6 + 2 * col), 1.0, 0.0).astype(F32)
    up_mask = jnp.where(has_up, 1.0, 0.0).astype(F32)
    down_mask = jnp.where(has_down, 1.0, 0.0).astype(F32)

    def frame_copy(t, slot):
        return pltpu.make_async_copy(frames.at[t], fbuf.at[slot], fsem.at[slot])

    for j in range(DEPTH):
        frame_copy(j, j).start()

    inputs = [pltpu.make_async_copy(src, dst, isem.at[i]) for i, (src, dst) in enumerate(
        ((h_hbm, h_in), (c_hbm, c_in), (wx_hbm, wx_in), (wh_hbm, wh_in), (bias_hbm, bias_in)))]
    for cp in inputs:
        cp.start()

    barrier = pltpu.get_barrier_semaphore()
    def toward(fn):
        def both(a, b):
            fn(a)
            fn(b)

        fn(FROM_SIDE)
        pl.when(has_up)(lambda: both(FROM_UP, FROM_DUP))
        pl.when(has_down)(lambda: both(FROM_DOWN, FROM_DDOWN))

    toward(lambda d: pl.semaphore_signal(barrier, inc=1, device_id=(grp, peers[d][1], peers[d][0]), device_id_type=MESH))

    def ingest(load, dst):
        def body(i, _):
            for u in range(4):
                q = i * 4 + u
                for s in range(2):
                    both = jnp.concatenate([load(s, 2 * q), load(s, 2 * q + 1)], axis=1).astype(F32)
                    dst[q, pl.ds(s, 32, stride=2), :] = both
            return 0
        lax.fori_loop(0, PAIRS // 4, body, 0)

    def wrap_first(ref, q):
        ref[q, AFTER, :] = ref[q, FIRST, :]

    nil = jnp.zeros((SUBL, 128), F32)
    for q in (0, 1, ROWS_ALL - 2, ROWS_ALL - 1):
        hs[q] = nil
        for j in range(2 * DEPTH):
            xs[j, q] = nil
    for q in (0, PAIRS + 1):
        cs[q] = nil[0:72]
    for q in range(PAIRS):
        cs[1 + q, CHALO, :] = nil[BEFORE]
        for j in (1, 2, 4, 5):
            xs[j, EDGE + q, BEFORE, :] = nil[BEFORE]
            xs[j, EDGE + q, HALO, :] = nil[BEFORE]

    strip_at = pl.multiple_of(8 + 56 * (1 - col), 8)
    cstrip_at = pl.multiple_of(56 * (1 - col), 8)
    cstrip_from = pl.multiple_of(60 * (1 - col), 4)
    cstrip_to = pl.multiple_of(64 + 4 * col, 4)

    def pack_rows(src, s_row):
        for p in range(HP):
            s_row[0, p] = src[EDGE + p, MID, :].astype(BF16)
            s_row[1, p] = src[EDGE + PAIRS - HP + p, MID, :].astype(BF16)

    def pack_cols(src, s_col, s_cor, part):
        for at, i in list(enumerate(COL_ORDER))[4 * part:4 * part + 4]:
            two = jnp.concatenate([src[EDGE + 2 * i, pl.ds(strip_at, 8), :],
                                   src[EDGE + 2 * i + 1, pl.ds(strip_at, 8), :]], axis=0).astype(BF16)
            s_col[at] = two
            if i == 0:
                s_cor[0] = two
            if i == PAIRS // 2 - 1:
                s_cor[1] = two

    def pack_narrow(src, s_row, s_col, s_cor):
        s_row[0, 0] = src[EDGE, MID, :].astype(BF16)
        s_row[1, 0] = src[EDGE + PAIRS - 1, MID, :].astype(BF16)
        for i in range(PAIRS // 4):
            s_col[i] = jnp.concatenate([src[EDGE + 4 * i + u, pl.ds(8 + cstrip_from, 4), :] for u in range(4)],
                                       axis=0).astype(BF16)
        for side_of, at in ((0, EDGE), (1, EDGE + PAIRS - 1)):
            edge = src[at, pl.ds(strip_at, 8), :]
            s_cor[side_of] = jnp.concatenate([edge, edge], axis=0).astype(BF16)

    def unpack_narrow(dst, get_row, get_col, get_cor):
        for i in range(PAIRS // 4):
            four = get_col(i).astype(F32)
            for u in range(4):
                strip = four[4 * u:4 * u + 4]
                dst[EDGE + 4 * i + u, pl.ds(8 + cstrip_to, 4), :] = strip
                dst[EDGE + 4 * i + u, pl.ds(cstrip_to - 64, 4), :] = strip
        for which, at, there in ((0, EDGE - 1, has_up), (1, EDGE + PAIRS, has_down)):
            strip = jnp.where(there, get_row(which).astype(F32), 0.0)
            dst[at, MID, :] = strip
            dst[at, AFTER, :] = strip[BEFORE]
            unpack_side(dst, at, jnp.where(there, get_cor(which).astype(F32)[BEFORE], 0.0))

    def unpack_side(dst, q, strip):
        strip = strip * col_mask
        dst[q, HALO, :] = strip
        dst[q, BEFORE, :] = strip

    def unpack_bf16(dst, get_row, get_col, get_cor):
        for at, i in enumerate(COL_ORDER):
            both = get_col(at).astype(F32)
            unpack_side(dst, EDGE + 2 * i, both[BEFORE])
            unpack_side(dst, EDGE + 2 * i + 1, both[8:16])

        for which, first, there in ((0, EDGE - HP, has_up), (1, EDGE + PAIRS, has_down)):
            both = jnp.where(there, get_cor(which).astype(F32), 0.0)
            for p in range(HP):
                strip = jnp.where(there, get_row(which, p).astype(F32), 0.0)
                dst[first + p, MID, :] = strip
                dst[first + p, AFTER, :] = strip[BEFORE]
                at = 2 - HP + p if which == 0 else p
                unpack_side(dst, first + p, both[8 * at:8 * at + 8])

    def ends(sends, recvs, d, m):
        (s_row, s_col, s_cor), (r_row, r_col, r_cor) = sends, recvs
        if d in (FROM_UP, FROM_DOWN):
            return s_row.at[d], r_row.at[m]
        if d == FROM_SIDE:
            return s_col, r_col
        return s_cor.at[d - FROM_DUP], r_cor.at[m - FROM_DUP]

    def remote(kind, b, j, d, m, src, dst):
        r, c = peers[d]
        return pltpu.make_async_remote_copy(
            src_ref=src, dst_ref=dst, send_sem=ssem.at[kind + j, d], recv_sem=rsem.at[b, kind + j, m],
            device_id=(grp, c, r), device_id_type=MESH)

    send_bufs = ((sx_row, sx_col, sx_cor), (sh_row, sh_col, sh_cor), (sc_row, sc_col, sc_cor))
    recv_bufs = ((rx_row, rx_col, rx_cor), (rh_row, rh_col, rh_cor), (rc_row, rc_col, rc_cor))

    def frame_ends(b, j, d, m):
        sends, recvs = ([x.at[b, j] for x in bufs[FRAME]] for bufs in (send_bufs, recv_bufs))
        src, dst = ends(sends, recvs, d, m)
        if j and d < FROM_SIDE:
            src, dst = src.at[pl.ds(0, 1)], dst.at[pl.ds(0, 1)]
        if j and d == FROM_SIDE:
            src, dst = src.at[pl.ds(0, 4)], dst.at[pl.ds(0, 4)]
        return src, dst

    def frame_out(b, j, d):
        remote(FRAME, b, 3 + j, d, MIRROR[d], *frame_ends(b, j, d, MIRROR[d])).start()

    def frame_in(b, j, d):
        remote(FRAME, b, 3 + j, d, d, *frame_ends(b, j, d, d)).wait_recv()

    def send_state(kind, b, d, half=None):
        sends, recvs = ([x.at[b] for x in bufs[kind]] for bufs in (send_bufs, recv_bufs))
        src, dst = ends(sends, recvs, d, MIRROR[d])
        if half is not None:
            src, dst = src.at[pl.ds(4 * half, 4)], dst.at[pl.ds(4 * half, 4)]
        remote(kind, b, 0, d, MIRROR[d], src, dst).start()

    def state_in(b, d):
        for kind in (HID, CELL):
            sends, recvs = ([x.at[b] for x in bufs[kind]] for bufs in (send_bufs, recv_bufs))
            src, dst = ends(sends, recvs, d, d)
            remote(kind, b, 0, d, d, src, dst).wait_recv()

    def drain(d):
        which = 0 if d < FROM_SIDE else 1 if d == FROM_SIDE else 2
        for kind in (HID, CELL):
            at = (slice(None),) + (() if d == FROM_SIDE else (d if d < FROM_SIDE else d - FROM_DUP,))
            remote(kind, 0, 0, d, d, send_bufs[kind][which].at[at], recv_bufs[kind][which].at[at]).wait_send()
        for j in range(DEPTH):
            frame_in(BLOCKS, j, d)
            if d == FROM_SIDE:
                at = (slice(None), j) + ((pl.ds(0, 4),) if j else ())
            elif d < FROM_SIDE:
                at = (slice(None), j, d) + ((pl.ds(0, 1),) if j else ())
            else:
                at = (slice(None), j, d - FROM_DUP)
            remote(FRAME, 0, 3 + j, d, d, send_bufs[FRAME][which].at[at], recv_bufs[FRAME][which].at[at]).wait_send()

    def send_state_cols(b, part):
        pack_cols(hs, sh_col.at[b], sh_cor.at[b], part)
        for at, i in list(enumerate(COL_ORDER))[4 * part:4 * part + 4]:
            for u in range(2):
                sc_col[b, at, 4 * u:4 * u + 4] = cs[1 + 2 * i + u, pl.ds(cstrip_from, 4), :]
        for kind in (HID, CELL):
            send_state(kind, b, FROM_SIDE, part)

    def send_state_rest(b):
        pack_rows(hs, sh_row.at[b])
        sc_row[b, 0] = cs[1, COWN, :]
        sc_row[b, 1] = cs[PAIRS, COWN, :]
        sc_cor[b, 0] = cs[1, pl.ds(cstrip_at, 8), :]
        sc_cor[b, 1] = cs[PAIRS, pl.ds(cstrip_at, 8), :]

        def out(d):
            if d != FROM_SIDE:
                for kind in (HID, CELL):
                    send_state(kind, b, d)

        toward(out)

    def receive_state(b):
        toward(lambda d: state_in(b, d))
        unpack_bf16(hs, lambda w, p: rh_row[b, w, p], lambda i: rh_col[b, i], lambda w: rh_cor[b, w])
        for at, i in enumerate(COL_ORDER):
            for u in range(2):
                cs[1 + 2 * i + u, pl.ds(cstrip_to, 4), :] = rc_col[b, at, 4 * u:4 * u + 4]
        for which, at, there in ((0, 0, has_up), (1, 1 + PAIRS, has_down)):
            cs[at, COWN, :] = jnp.where(there, rc_row[b, which], 0.0)
            cs[at, CHALO, :] = jnp.where(there, rc_cor[b, which], 0.0)

    def plane(b, j):
        return xs.at[lax.rem(b, 2) * DEPTH + j]

    def take_frame(b, j):
        dst = plane(b, j)
        for q in range(PAIRS):
            for s in range(2):
                both = jnp.concatenate([fbuf[j, s, 2 * q], fbuf[j, s, 2 * q + 1]], axis=1).astype(F32)
                dst[EDGE + q, pl.ds(8 + s, 32, stride=2), :] = both
            wrap_first(dst, EDGE + q)
        pack_frame(b, j)

    def pack_frame(b, j):
        if j:
            pack_narrow(plane(b, j), sx_row.at[b, j], sx_col.at[b, j], sx_cor.at[b, j])
            return
        pack_rows(plane(b, j), sx_row.at[b, j])
        for part in range(2):
            pack_cols(plane(b, j), sx_col.at[b, j], sx_cor.at[b, j], part)

    def tasks(j):
        first, count, width = region(j)
        if count == 18:
            lists = ((1, 2, 3, 16, 17, 18), (4, 5, 6, 13, 14, 15), (7, 8, 9, 10, 11, 12))
        else:
            lists = ((2, 3, 4, 5, 14, 15, 16, 17), (6, 7, 8, 9, 10, 11, 12, 13))
        out, base = [], 0
        for pairs in lists:
            out.append((j, pairs, width, base))
            base += len(pairs) * width
        return out

    def product(src, task, w):
        _, pairs, width, _ = task
        low = (lane < 64)[0:width]
        total = None
        for dx in range(3):
            at = pl.ds(6 + 2 * dx, width)
            r = {q: src[q, at, :] for q in sorted({p + e for p in pairs for e in (-1, 0, 1)})}
            own = jnp.concatenate([r[q] for q in pairs], axis=0).astype(BF16)
            near = jnp.concatenate([jnp.where(low, r[q + 1], r[q - 1]) for q in pairs], axis=0).astype(BF16)
            part = jnp.dot(jnp.concatenate([own, near], axis=1), w[dx * 256:dx * 256 + 256, :], preferred_element_type=F32)
            total = part if total is None else total + part
        return total

    def unpack_frame(b, j):
        if j:
            unpack_narrow(plane(b, j), lambda w: rx_row[b, j, w, 0], lambda i: rx_col[b, j, i], lambda w: rx_cor[b, j, w])
            return
        unpack_bf16(plane(b, j), lambda w, p: rx_row[b, j, w, p], lambda i: rx_col[b, j, i], lambda w: rx_cor[b, j, w])

    def x_gates(src, slot, task):
        j, pairs, width, at = task
        xg[j, at:at + len(pairs) * width, :] = product(src, task, wx) + bias[...]

    all_tasks = [t for j in range(DEPTH) for t in tasks(j)]
    def frames_wait():
        for j in range(DEPTH):
            frame_copy(0, j).wait()

    def fetch(b):
        for j in range(DEPTH):
            frame_copy(b * DEPTH + j, j).start()

    def h_gates(src, slot, task):
        j, pairs, width, base = task
        rows = len(pairs) * width
        gts[slot, 0:rows, :] = product(src, task, wh) + xg[j, base:base + rows, :]

    def cells(slot, task, t):
        j, pairs, width, _ = task
        for q, at in enumerate(pairs):
            rows_q = pl.ds(q * width, width)
            gi, gf, go, gg = (gts[slot, rows_q, 128 * i:128 * i + 128] for i in range(4))
            c_old = cs[at - 1, 0:width, :]
            ti, tf, to = jnp.tanh(0.5 * gi), jnp.tanh(0.5 * gf), jnp.tanh(0.5 * go)
            c_new = 0.5 * ((tf + 1.0) * c_old + (ti + 1.0) * jnp.tanh(gg))
            cs[at - 1, 0:width, :] = c_new
            h_new = 0.5 * (to + 1.0) * jnp.tanh(c_new)
            if at < EDGE:
                h_new = h_new * up_mask
            if at >= EDGE + PAIRS:
                h_new = h_new * down_mask
            hs[at, MID, :] = h_new[0:OWN]
            hs[at, AFTER, :] = h_new[BEFORE]
            if width == 72:
                unpack_side(hs, at, h_new[64:72])
            if EDGE <= at < EDGE + PAIRS:
                for s in range(2):
                    both = hs[at, pl.ds(8 + s, 32, stride=2), :].astype(BF16)
                    h_out[t, s, 2 * (at - EDGE)] = both[:, LEFT]
                    h_out[t, s, 2 * (at - EDGE) + 1] = both[:, RIGHT]

    def run(hid_block, x_block):
        todo = []
        if hid_block is not None:
            todo += [(hs, t, True) for t in all_tasks]
        if x_block is not None:
            todo += [(plane(x_block, t[0]), t, False) for t in all_tasks]
        def ahead(i):
            src, task, hidden = todo[i]
            (h_gates if hidden else x_gates)(src, i % 2, task)

        ahead(0)
        for i, (src, task, hidden) in enumerate(todo):
            n = i % len(all_tasks)
            if hidden and x_block is not None and n + 1 == len(all_tasks):
                for j in range(DEPTH):
                    unpack_frame(x_block, j)
            if i + 1 < len(todo):
                ahead(i + 1)
            if hidden:
                cells(i % 2, task, hid_block * DEPTH + task[0])
                if x_block is None:
                    continue
                if n < DEPTH:
                    take_frame(x_block + 1, n)
                if n + 2 == len(all_tasks):
                    send_state_cols(hid_block + 1, 0)
                    send_state_rest(hid_block + 1)
                    toward(lambda d: [frame_in(x_block, j, d) for j in range(DEPTH)])
                if n + 1 == len(all_tasks):
                    send_state_cols(hid_block + 1, 1)
                    toward(lambda d: [frame_out(x_block + 1, j, d) for j in range(DEPTH)])

    def weights(src, dst):
        zero = jnp.zeros((64, 64), BF16)
        for dx in range(3):
            for k, q in enumerate((0, 1, 2, -1)):
                for g in range(4):
                    parts = []
                    for p in range(2):
                        dy = q - p + 1
                        parts.append(src[dy, dx, :, 64 * g:64 * g + 64] if 0 <= dy <= 2 else zero)
                    dst[dx * 256 + k * 64:dx * 256 + k * 64 + 64, 128 * g:128 * g + 128] = jnp.concatenate(parts, axis=1)

    for j in range(DEPTH):
        frame_copy(0, j).wait()
        take_frame(0, j)
        frame_copy(DEPTH + j, j).start()
    for j in range(DEPTH):
        if j == 0:
            pl.semaphore_wait(barrier, 3 + 2 * (has_up & has_down).astype(jnp.int32))
        toward(lambda d: frame_out(0, j, d))
    for cp in inputs:
        cp.wait()
    ingest(lambda s, r: h_in[s, r], hs.at[pl.ds(EDGE, PAIRS), pl.ds(8, OWN)])
    ingest(lambda s, r: c_in[s, r], cs.at[pl.ds(1, PAIRS), pl.ds(0, OWN)])
    for q in range(PAIRS):
        wrap_first(hs, EDGE + q)
    for part in range(2):
        send_state_cols(0, part)
    send_state_rest(0)
    weights(wx_in, wx)
    weights(wh_in, wh)
    for g in range(4):
        piece = bias_in[:, 64 * g:64 * g + 64]
        bias[:, 128 * g:128 * g + 128] = jnp.concatenate([piece, piece], axis=1)
    frames_wait()
    for j in range(DEPTH):
        take_frame(1, j)
    toward(lambda d: [frame_out(1, j, d) for j in range(DEPTH)])
    fetch(2)
    for j in range(DEPTH):
        toward(lambda d: frame_in(0, j, d))
        unpack_frame(0, j)
        for task in tasks(j):
            x_gates(plane(0, j), 0, task)

    def block(b, _):
        pl.when(b + 2 < BLOCKS)(frames_wait)
        receive_state(b)
        run(b, b + 1)
        pl.when(b + 3 < BLOCKS)(lambda: fetch(b + 3))
        return 0

    lax.fori_loop(0, BLOCKS - 1, block, 0)
    receive_state(BLOCKS - 1)
    run(BLOCKS - 1, None)

    for q in range(PAIRS):
        for s in range(2):
            both = cs[1 + q, pl.ds(s, 32, stride=2), :]
            c_out[s, 2 * q] = both[:, LEFT]
            c_out[s, 2 * q + 1] = both[:, RIGHT]

    toward(drain)


def write_out(h, c, h_out, c_out, sem):
    copies = [pltpu.make_async_copy(h.at[t], h_out.at[t], sem.at[t]) for t in range(STEPS)]
    copies.append(pltpu.make_async_copy(c, c_out, sem.at[STEPS]))
    for cp in copies:
        cp.start()
    for cp in copies:
        cp.wait()


def solution(mesh):
    frame_spec = P(None, "batch", "rows", "cols", None)
    state_spec = P("batch", "rows", "cols", None)

    def local_run(frames, w_x, w_h, gate_bias, h_init, c_init):
        vmem = pl.BlockSpec(memory_space=pltpu.VMEM)
        hbm = pl.BlockSpec(memory_space=pltpu.HBM)
        most = max(region(j)[1] * region(j)[2] for j in range(DEPTH))
        strips = [
            [(BLOCKS, DEPTH, 2, HP, OWN, 128), (BLOCKS, DEPTH, 8, 16, 128), (BLOCKS, DEPTH, 2, 16, 128)],
            [(BLOCKS, 2, HP, OWN, 128), (BLOCKS, 8, 16, 128), (BLOCKS, 2, 16, 128)],
            [(BLOCKS, 2, OWN, 128), (BLOCKS, PAIRS // 2, 8, 128), (BLOCKS, 2, 8, 128)],
        ]
        strips[0] = [(s[0] + 1,) + s[1:] for s in strips[0]]
        strip_bufs = [pltpu.VMEM(s, BF16 if k < 2 else F32) for k in range(3) for s in strips[k]]
        h_pairs, c_pairs = pl.pallas_call(
            kernel,
            out_shape=(pltpu.VMEM(frames.shape, BF16), pltpu.VMEM(c_init.shape, F32)),
            in_specs=[hbm] * 6,
            out_specs=(vmem, vmem),
            scratch_shapes=[
                pltpu.VMEM((DEPTH,) + h_init.shape, BF16),
                pltpu.VMEM(w_x.shape, BF16),
                pltpu.VMEM(w_h.shape, BF16),
                pltpu.VMEM((1, 256), F32),
                pltpu.VMEM(h_init.shape, BF16),
                pltpu.VMEM(c_init.shape, F32),
                pltpu.VMEM((2 * DEPTH, ROWS_ALL, SUBL, 128), F32),
                pltpu.VMEM((ROWS_ALL, SUBL, 128), F32),
                pltpu.VMEM((PAIRS + 2, 72, 128), F32),
                pltpu.VMEM((DEPTH, most, 512), F32),
                pltpu.VMEM((2, 512, 512), F32),
                pltpu.VMEM((768, 512), BF16),
                pltpu.VMEM((768, 512), BF16),
                pltpu.VMEM((1, 512), F32),
                *strip_bufs, *strip_bufs,
                pltpu.SemaphoreType.DMA((DEPTH,)),
                pltpu.SemaphoreType.DMA((5,)),
                pltpu.SemaphoreType.DMA((3 + DEPTH, 5)),
                pltpu.SemaphoreType.DMA((BLOCKS + 1, 3 + DEPTH, 5)),
            ],
            compiler_params=pltpu.CompilerParams(collective_id=0, has_side_effects=True, vmem_limit_bytes=56 * 2**20),
        )(frames, w_x, w_h, gate_bias.reshape(1, 256), h_init, c_init)
        return pl.pallas_call(
            write_out,
            out_shape=(jax.ShapeDtypeStruct(frames.shape, BF16), jax.ShapeDtypeStruct(c_init.shape, F32)),
            in_specs=[vmem, vmem],
            out_specs=(hbm, hbm),
            scratch_shapes=[pltpu.SemaphoreType.DMA((STEPS + 1,))],
            compiler_params=pltpu.CompilerParams(vmem_limit_bytes=16 * 2**20),
        )(h_pairs, c_pairs)

    return jax.shard_map(local_run, mesh=mesh, in_specs=(frame_spec, P(), P(), P(), state_spec, state_spec),
                         out_specs=(frame_spec, state_spec), check_vma=False)
```

```python
import functools

import jax
import jax.numpy as jnp
from jax import lax
from jax.experimental import pallas as pl
from jax.experimental.pallas import tpu as pltpu
from jax.sharding import PartitionSpec as P

MESH = pl.DeviceIdType.MESH
F32, BF16 = jnp.float32, jnp.bfloat16

DEPTH = 3
STEPS = 12
BLOCKS = STEPS // DEPTH
PAIRS = 16
OWN = 64
EDGE = 2
HP = -(-DEPTH // 2)
ROWS_ALL = PAIRS + 2 * EDGE
SUBL = 88
FROM_UP, FROM_DOWN, FROM_SIDE, FROM_DUP, FROM_DDOWN = DIRS = range(5)
MIRROR = (FROM_DOWN, FROM_UP, FROM_SIDE, FROM_DDOWN, FROM_DUP)
FRAME, HID, CELL = range(3)
MID, HALO = slice(8, 72), slice(72, 80)
BEFORE, AFTER = slice(0, 8), slice(80, 88)
FIRST, COWN, CHALO = slice(8, 16), slice(0, 64), slice(64, 72)
LEFT, RIGHT = slice(0, 64), slice(64, 128)
COL_ORDER = (0, 1, 6, 7, 2, 3, 4, 5)


def region(j):
    halo = DEPTH - 1 - j
    extra = -(-halo // 2)
    return EDGE - extra, PAIRS + 2 * extra, 72 if halo else OWN


def kernel(frames, wx_hbm, wh_hbm, bias_hbm, h_hbm, c_hbm, h_out, c_out,
           fbuf, wx_in, wh_in, bias_in, h_in, c_in, xs, hs, cs, xg, gts, wx, wh, bias,
           sx_row, sx_col, sx_cor, sh_row, sh_col, sh_cor, sc_row, sc_col, sc_cor,
           rx_row, rx_col, rx_cor, rh_row, rh_col, rh_cor, rc_row, rc_col, rc_cor,
           fsem, isem, ssem, rsem):
    row, col, grp = lax.axis_index("rows"), lax.axis_index("cols"), lax.axis_index("batch")
    n_rows = lax.axis_size("rows")
    side = 1 - col
    has_up, has_down = row > 0, row < n_rows - 1
    above, below = lax.rem(row + n_rows - 1, n_rows), lax.rem(row + 1, n_rows)
    peers = ((above, col), (below, col), (row, side), (above, side), (below, side))

    lane = lax.broadcasted_iota(jnp.int32, (72, 128), 1)
    subl = lax.broadcasted_iota(jnp.int32, (8, 128), 0)
    col_mask = jnp.where((subl + 2 * (1 - col) >= 2) & (subl < 6 + 2 * col), 1.0, 0.0).astype(F32)
    up_mask = jnp.where(has_up, 1.0, 0.0).astype(F32)
    down_mask = jnp.where(has_down, 1.0, 0.0).astype(F32)

    def frame_copy(t, slot):
        return pltpu.make_async_copy(frames.at[t], fbuf.at[slot], fsem.at[slot])

    for j in range(DEPTH):
        frame_copy(j, j).start()

    inputs = [pltpu.make_async_copy(src, dst, isem.at[i]) for i, (src, dst) in enumerate(
        ((h_hbm, h_in), (c_hbm, c_in), (wx_hbm, wx_in), (wh_hbm, wh_in), (bias_hbm, bias_in)))]
    for cp in inputs:
        cp.start()

    barrier = pltpu.get_barrier_semaphore()
    def toward(fn):
        def both(a, b):
            fn(a)
            fn(b)

        fn(FROM_SIDE)
        pl.when(has_up)(lambda: both(FROM_UP, FROM_DUP))
        pl.when(has_down)(lambda: both(FROM_DOWN, FROM_DDOWN))

    toward(lambda d: pl.semaphore_signal(barrier, inc=1, device_id=(grp, peers[d][1], peers[d][0]), device_id_type=MESH))

    def ingest(load, dst):
        def body(i, _):
            for u in range(4):
                q = i * 4 + u
                for s in range(2):
                    both = jnp.concatenate([load(s, 2 * q), load(s, 2 * q + 1)], axis=1).astype(F32)
                    dst[q, pl.ds(s, 32, stride=2), :] = both
            return 0
        lax.fori_loop(0, PAIRS // 4, body, 0)

    def wrap_first(ref, q):
        ref[q, AFTER, :] = ref[q, FIRST, :]

    nil = jnp.zeros((SUBL, 128), F32)
    for q in (0, 1, ROWS_ALL - 2, ROWS_ALL - 1):
        hs[q] = nil
        for j in range(2 * DEPTH):
            xs[j, q] = nil
    for q in (0, PAIRS + 1):
        cs[q] = nil[0:72]
    for q in range(PAIRS):
        cs[1 + q, CHALO, :] = nil[BEFORE]
        for j in (1, 2, 4, 5):
            xs[j, EDGE + q, BEFORE, :] = nil[BEFORE]
            xs[j, EDGE + q, HALO, :] = nil[BEFORE]

    strip_at = pl.multiple_of(8 + 56 * (1 - col), 8)
    cstrip_at = pl.multiple_of(56 * (1 - col), 8)
    cstrip_from = pl.multiple_of(60 * (1 - col), 4)
    cstrip_to = pl.multiple_of(64 + 4 * col, 4)

    def pack_rows(src, s_row):
        for p in range(HP):
            s_row[0, p] = src[EDGE + p, MID, :].astype(BF16)
            s_row[1, p] = src[EDGE + PAIRS - HP + p, MID, :].astype(BF16)

    def pack_cols(src, s_col, s_cor, part):
        for at, i in list(enumerate(COL_ORDER))[4 * part:4 * part + 4]:
            two = jnp.concatenate([src[EDGE + 2 * i, pl.ds(strip_at, 8), :],
                                   src[EDGE + 2 * i + 1, pl.ds(strip_at, 8), :]], axis=0).astype(BF16)
            s_col[at] = two
            if i == 0:
                s_cor[0] = two
            if i == PAIRS // 2 - 1:
                s_cor[1] = two

    def pack_narrow(src, s_row, s_col, s_cor):
        s_row[0, 0] = src[EDGE, MID, :].astype(BF16)
        s_row[1, 0] = src[EDGE + PAIRS - 1, MID, :].astype(BF16)
        for i in range(PAIRS // 4):
            s_col[i] = jnp.concatenate([src[EDGE + 4 * i + u, pl.ds(8 + cstrip_from, 4), :] for u in range(4)],
                                       axis=0).astype(BF16)
        for side_of, at in ((0, EDGE), (1, EDGE + PAIRS - 1)):
            edge = src[at, pl.ds(strip_at, 8), :]
            s_cor[side_of] = jnp.concatenate([edge, edge], axis=0).astype(BF16)

    def unpack_narrow(dst, get_row, get_col, get_cor):
        for i in range(PAIRS // 4):
            four = get_col(i).astype(F32)
            for u in range(4):
                strip = four[4 * u:4 * u + 4]
                dst[EDGE + 4 * i + u, pl.ds(8 + cstrip_to, 4), :] = strip
                dst[EDGE + 4 * i + u, pl.ds(cstrip_to - 64, 4), :] = strip
        for which, at, there in ((0, EDGE - 1, has_up), (1, EDGE + PAIRS, has_down)):
            strip = jnp.where(there, get_row(which).astype(F32), 0.0)
            dst[at, MID, :] = strip
            dst[at, AFTER, :] = strip[BEFORE]
            unpack_side(dst, at, jnp.where(there, get_cor(which).astype(F32)[BEFORE], 0.0))

    def unpack_side(dst, q, strip):
        strip = strip * col_mask
        dst[q, HALO, :] = strip
        dst[q, BEFORE, :] = strip

    def unpack_bf16(dst, get_row, get_col, get_cor):
        for at, i in enumerate(COL_ORDER):
            both = get_col(at).astype(F32)
            unpack_side(dst, EDGE + 2 * i, both[BEFORE])
            unpack_side(dst, EDGE + 2 * i + 1, both[8:16])

        for which, first, there in ((0, EDGE - HP, has_up), (1, EDGE + PAIRS, has_down)):
            both = jnp.where(there, get_cor(which).astype(F32), 0.0)
            for p in range(HP):
                strip = jnp.where(there, get_row(which, p).astype(F32), 0.0)
                dst[first + p, MID, :] = strip
                dst[first + p, AFTER, :] = strip[BEFORE]
                at = 2 - HP + p if which == 0 else p
                unpack_side(dst, first + p, both[8 * at:8 * at + 8])

    def ends(sends, recvs, d, m):
        (s_row, s_col, s_cor), (r_row, r_col, r_cor) = sends, recvs
        if d in (FROM_UP, FROM_DOWN):
            return s_row.at[d], r_row.at[m]
        if d == FROM_SIDE:
            return s_col, r_col
        return s_cor.at[d - FROM_DUP], r_cor.at[m - FROM_DUP]

    def remote(kind, b, j, d, m, src, dst):
        r, c = peers[d]
        return pltpu.make_async_remote_copy(
            src_ref=src, dst_ref=dst, send_sem=ssem.at[kind + j, d], recv_sem=rsem.at[b, kind + j, m],
            device_id=(grp, c, r), device_id_type=MESH)

    send_bufs = ((sx_row, sx_col, sx_cor), (sh_row, sh_col, sh_cor), (sc_row, sc_col, sc_cor))
    recv_bufs = ((rx_row, rx_col, rx_cor), (rh_row, rh_col, rh_cor), (rc_row, rc_col, rc_cor))

    def frame_ends(b, j, d, m):
        sends, recvs = ([x.at[b, j] for x in bufs[FRAME]] for bufs in (send_bufs, recv_bufs))
        src, dst = ends(sends, recvs, d, m)
        if j and d < FROM_SIDE:
            src, dst = src.at[pl.ds(0, 1)], dst.at[pl.ds(0, 1)]
        if j and d == FROM_SIDE:
            src, dst = src.at[pl.ds(0, 4)], dst.at[pl.ds(0, 4)]
        return src, dst

    def frame_out(b, j, d):
        remote(FRAME, b, 3 + j, d, MIRROR[d], *frame_ends(b, j, d, MIRROR[d])).start()

    def frame_in(b, j, d):
        remote(FRAME, b, 3 + j, d, d, *frame_ends(b, j, d, d)).wait_recv()

    def send_state(kind, b, d, half=None):
        sends, recvs = ([x.at[b] for x in bufs[kind]] for bufs in (send_bufs, recv_bufs))
        src, dst = ends(sends, recvs, d, MIRROR[d])
        if half is not None:
            src, dst = src.at[pl.ds(4 * half, 4)], dst.at[pl.ds(4 * half, 4)]
        remote(kind, b, 0, d, MIRROR[d], src, dst).start()

    def state_in(b, d):
        for kind in (HID, CELL):
            sends, recvs = ([x.at[b] for x in bufs[kind]] for bufs in (send_bufs, recv_bufs))
            src, dst = ends(sends, recvs, d, d)
            remote(kind, b, 0, d, d, src, dst).wait_recv()

    def drain(d):
        which = 0 if d < FROM_SIDE else 1 if d == FROM_SIDE else 2
        for kind in (HID, CELL):
            at = (slice(None),) + (() if d == FROM_SIDE else (d if d < FROM_SIDE else d - FROM_DUP,))
            remote(kind, 0, 0, d, d, send_bufs[kind][which].at[at], recv_bufs[kind][which].at[at]).wait_send()
        for j in range(DEPTH):
            frame_in(BLOCKS, j, d)
            if d == FROM_SIDE:
                at = (slice(None), j) + ((pl.ds(0, 4),) if j else ())
            elif d < FROM_SIDE:
                at = (slice(None), j, d) + ((pl.ds(0, 1),) if j else ())
            else:
                at = (slice(None), j, d - FROM_DUP)
            remote(FRAME, 0, 3 + j, d, d, send_bufs[FRAME][which].at[at], recv_bufs[FRAME][which].at[at]).wait_send()

    def send_state_cols(b, part):
        pack_cols(hs, sh_col.at[b], sh_cor.at[b], part)
        for at, i in list(enumerate(COL_ORDER))[4 * part:4 * part + 4]:
            for u in range(2):
                sc_col[b, at, 4 * u:4 * u + 4] = cs[1 + 2 * i + u, pl.ds(cstrip_from, 4), :]
        for kind in (HID, CELL):
            send_state(kind, b, FROM_SIDE, part)

    def send_state_rest(b):
        pack_rows(hs, sh_row.at[b])
        sc_row[b, 0] = cs[1, COWN, :]
        sc_row[b, 1] = cs[PAIRS, COWN, :]
        sc_cor[b, 0] = cs[1, pl.ds(cstrip_at, 8), :]
        sc_cor[b, 1] = cs[PAIRS, pl.ds(cstrip_at, 8), :]

        def out(d):
            if d != FROM_SIDE:
                for kind in (HID, CELL):
                    send_state(kind, b, d)

        toward(out)

    def receive_state(b):
        toward(lambda d: state_in(b, d))
        unpack_bf16(hs, lambda w, p: rh_row[b, w, p], lambda i: rh_col[b, i], lambda w: rh_cor[b, w])
        for at, i in enumerate(COL_ORDER):
            for u in range(2):
                cs[1 + 2 * i + u, pl.ds(cstrip_to, 4), :] = rc_col[b, at, 4 * u:4 * u + 4]
        for which, at, there in ((0, 0, has_up), (1, 1 + PAIRS, has_down)):
            cs[at, COWN, :] = jnp.where(there, rc_row[b, which], 0.0)
            cs[at, CHALO, :] = jnp.where(there, rc_cor[b, which], 0.0)

    def plane(b, j):
        return xs.at[lax.rem(b, 2) * DEPTH + j]

    def take_frame(b, j):
        dst = plane(b, j)
        for q in range(PAIRS):
            for s in range(2):
                both = jnp.concatenate([fbuf[j, s, 2 * q], fbuf[j, s, 2 * q + 1]], axis=1).astype(F32)
                dst[EDGE + q, pl.ds(8 + s, 32, stride=2), :] = both
            wrap_first(dst, EDGE + q)
        pack_frame(b, j)

    def pack_frame(b, j):
        if j:
            pack_narrow(plane(b, j), sx_row.at[b, j], sx_col.at[b, j], sx_cor.at[b, j])
            return
        pack_rows(plane(b, j), sx_row.at[b, j])
        for part in range(2):
            pack_cols(plane(b, j), sx_col.at[b, j], sx_cor.at[b, j], part)

    def tasks(j):
        first, count, width = region(j)
        if count == 18:
            lists = ((1, 2, 3, 16, 17, 18), (4, 5, 6, 13, 14, 15), (7, 8, 9, 10, 11, 12))
        else:
            lists = ((2, 3, 4, 5, 14, 15, 16, 17), (6, 7, 8, 9, 10, 11, 12, 13))
        out, base = [], 0
        for pairs in lists:
            out.append((j, pairs, width, base))
            base += len(pairs) * width
        return out

    def product(src, task, w):
        _, pairs, width, _ = task
        low = (lane < 64)[0:width]
        total = None
        for dx in range(3):
            at = pl.ds(6 + 2 * dx, width)
            r = {q: src[q, at, :] for q in sorted({p + e for p in pairs for e in (-1, 0, 1)})}
            own = jnp.concatenate([r[q] for q in pairs], axis=0).astype(BF16)
            near = jnp.concatenate([jnp.where(low, r[q + 1], r[q - 1]) for q in pairs], axis=0).astype(BF16)
            part = jnp.dot(jnp.concatenate([own, near], axis=1), w[dx * 256:dx * 256 + 256, :], preferred_element_type=F32)
            total = part if total is None else total + part
        return total

    def unpack_frame(b, j):
        if j:
            unpack_narrow(plane(b, j), lambda w: rx_row[b, j, w, 0], lambda i: rx_col[b, j, i], lambda w: rx_cor[b, j, w])
            return
        unpack_bf16(plane(b, j), lambda w, p: rx_row[b, j, w, p], lambda i: rx_col[b, j, i], lambda w: rx_cor[b, j, w])

    def x_gates(src, slot, task):
        j, pairs, width, at = task
        xg[j, at:at + len(pairs) * width, :] = product(src, task, wx) + bias[...]

    all_tasks = [t for j in range(DEPTH) for t in tasks(j)]
    def frames_wait():
        for j in range(DEPTH):
            frame_copy(0, j).wait()

    def fetch(b):
        for j in range(DEPTH):
            frame_copy(b * DEPTH + j, j).start()

    def h_gates(src, slot, task):
        j, pairs, width, base = task
        rows = len(pairs) * width
        gts[slot, 0:rows, :] = product(src, task, wh) + xg[j, base:base + rows, :]

    def cells(slot, task, t):
        j, pairs, width, _ = task
        for q, at in enumerate(pairs):
            rows_q = pl.ds(q * width, width)
            gi, gf, go, gg = (gts[slot, rows_q, 128 * i:128 * i + 128] for i in range(4))
            c_old = cs[at - 1, 0:width, :]
            ti, tf, to = jnp.tanh(0.5 * gi), jnp.tanh(0.5 * gf), jnp.tanh(0.5 * go)
            c_new = 0.5 * ((tf + 1.0) * c_old + (ti + 1.0) * jnp.tanh(gg))
            cs[at - 1, 0:width, :] = c_new
            h_new = 0.5 * (to + 1.0) * jnp.tanh(c_new)
            if at < EDGE:
                h_new = h_new * up_mask
            if at >= EDGE + PAIRS:
                h_new = h_new * down_mask
            hs[at, MID, :] = h_new[0:OWN]
            hs[at, AFTER, :] = h_new[BEFORE]
            if width == 72:
                unpack_side(hs, at, h_new[64:72])
            if EDGE <= at < EDGE + PAIRS:
                for s in range(2):
                    both = hs[at, pl.ds(8 + s, 32, stride=2), :].astype(BF16)
                    h_out[t, s, 2 * (at - EDGE)] = both[:, LEFT]
                    h_out[t, s, 2 * (at - EDGE) + 1] = both[:, RIGHT]

    def run(hid_block, x_block):
        todo = []
        if hid_block is not None:
            todo += [(hs, t, True) for t in all_tasks]
        if x_block is not None:
            todo += [(plane(x_block, t[0]), t, False) for t in all_tasks]
        def ahead(i):
            src, task, hidden = todo[i]
            (h_gates if hidden else x_gates)(src, i % 2, task)

        ahead(0)
        for i, (src, task, hidden) in enumerate(todo):
            n = i % len(all_tasks)
            if hidden and x_block is not None and n + 1 == len(all_tasks):
                for j in range(DEPTH):
                    unpack_frame(x_block, j)
            if i + 1 < len(todo):
                ahead(i + 1)
            if hidden:
                cells(i % 2, task, hid_block * DEPTH + task[0])
                if x_block is None:
                    continue
                if n % 2 and n < 2 * DEPTH:
                    take_frame(x_block + 1, n // 2)
                if n + 2 == len(all_tasks):
                    send_state_cols(hid_block + 1, 0)
                    send_state_rest(hid_block + 1)
                    toward(lambda d: [frame_in(x_block, j, d) for j in range(DEPTH)])
                if n + 1 == len(all_tasks):
                    send_state_cols(hid_block + 1, 1)
                    toward(lambda d: [frame_out(x_block + 1, j, d) for j in range(DEPTH)])

    def weights(src, dst):
        zero = jnp.zeros((64, 64), BF16)
        for dx in range(3):
            for k, q in enumerate((0, 1, 2, -1)):
                for g in range(4):
                    parts = []
                    for p in range(2):
                        dy = q - p + 1
                        parts.append(src[dy, dx, :, 64 * g:64 * g + 64] if 0 <= dy <= 2 else zero)
                    dst[dx * 256 + k * 64:dx * 256 + k * 64 + 64, 128 * g:128 * g + 128] = jnp.concatenate(parts, axis=1)

    for j in range(DEPTH):
        frame_copy(0, j).wait()
        take_frame(0, j)
        frame_copy(DEPTH + j, j).start()
    for j in range(DEPTH):
        if j == 0:
            pl.semaphore_wait(barrier, 3 + 2 * (has_up & has_down).astype(jnp.int32))
        toward(lambda d: frame_out(0, j, d))
    for cp in inputs:
        cp.wait()
    ingest(lambda s, r: h_in[s, r], hs.at[pl.ds(EDGE, PAIRS), pl.ds(8, OWN)])
    ingest(lambda s, r: c_in[s, r], cs.at[pl.ds(1, PAIRS), pl.ds(0, OWN)])
    for q in range(PAIRS):
        wrap_first(hs, EDGE + q)
    for part in range(2):
        send_state_cols(0, part)
    send_state_rest(0)
    weights(wx_in, wx)
    weights(wh_in, wh)
    for g in range(4):
        piece = bias_in[:, 64 * g:64 * g + 64]
        bias[:, 128 * g:128 * g + 128] = jnp.concatenate([piece, piece], axis=1)
    frames_wait()
    for j in range(DEPTH):
        take_frame(1, j)
    toward(lambda d: [frame_out(1, j, d) for j in range(DEPTH)])
    fetch(2)
    for j in range(DEPTH):
        toward(lambda d: frame_in(0, j, d))
        unpack_frame(0, j)
        for task in tasks(j):
            x_gates(plane(0, j), 0, task)

    def block(b, _):
        pl.when(b + 2 < BLOCKS)(frames_wait)
        receive_state(b)
        run(b, b + 1)
        pl.when(b + 3 < BLOCKS)(lambda: fetch(b + 3))
        return 0

    lax.fori_loop(0, BLOCKS - 1, block, 0)
    receive_state(BLOCKS - 1)
    run(BLOCKS - 1, None)

    for q in range(PAIRS):
        for s in range(2):
            both = cs[1 + q, pl.ds(s, 32, stride=2), :]
            c_out[s, 2 * q] = both[:, LEFT]
            c_out[s, 2 * q + 1] = both[:, RIGHT]

    toward(drain)


def write_out(h, c, h_out, c_out, sem):
    copies = [pltpu.make_async_copy(h.at[t], h_out.at[t], sem.at[t]) for t in range(STEPS)]
    copies.append(pltpu.make_async_copy(c, c_out, sem.at[STEPS]))
    for cp in copies:
        cp.start()
    for cp in copies:
        cp.wait()


def solution(mesh):
    frame_spec = P(None, "batch", "rows", "cols", None)
    state_spec = P("batch", "rows", "cols", None)

    def local_run(frames, w_x, w_h, gate_bias, h_init, c_init):
        vmem = pl.BlockSpec(memory_space=pltpu.VMEM)
        hbm = pl.BlockSpec(memory_space=pltpu.HBM)
        most = max(region(j)[1] * region(j)[2] for j in range(DEPTH))
        strips = [
            [(BLOCKS, DEPTH, 2, HP, OWN, 128), (BLOCKS, DEPTH, 8, 16, 128), (BLOCKS, DEPTH, 2, 16, 128)],
            [(BLOCKS, 2, HP, OWN, 128), (BLOCKS, 8, 16, 128), (BLOCKS, 2, 16, 128)],
            [(BLOCKS, 2, OWN, 128), (BLOCKS, PAIRS // 2, 8, 128), (BLOCKS, 2, 8, 128)],
        ]
        strips[0] = [(s[0] + 1,) + s[1:] for s in strips[0]]
        strip_bufs = [pltpu.VMEM(s, BF16 if k < 2 else F32) for k in range(3) for s in strips[k]]
        h_pairs, c_pairs = pl.pallas_call(
            kernel,
            out_shape=(pltpu.VMEM(frames.shape, BF16), pltpu.VMEM(c_init.shape, F32)),
            in_specs=[hbm] * 6,
            out_specs=(vmem, vmem),
            scratch_shapes=[
                pltpu.VMEM((DEPTH,) + h_init.shape, BF16),
                pltpu.VMEM(w_x.shape, BF16),
                pltpu.VMEM(w_h.shape, BF16),
                pltpu.VMEM((1, 256), F32),
                pltpu.VMEM(h_init.shape, BF16),
                pltpu.VMEM(c_init.shape, F32),
                pltpu.VMEM((2 * DEPTH, ROWS_ALL, SUBL, 128), F32),
                pltpu.VMEM((ROWS_ALL, SUBL, 128), F32),
                pltpu.VMEM((PAIRS + 2, 72, 128), F32),
                pltpu.VMEM((DEPTH, most, 512), F32),
                pltpu.VMEM((2, 512, 512), F32),
                pltpu.VMEM((768, 512), BF16),
                pltpu.VMEM((768, 512), BF16),
                pltpu.VMEM((1, 512), F32),
                *strip_bufs, *strip_bufs,
                pltpu.SemaphoreType.DMA((DEPTH,)),
                pltpu.SemaphoreType.DMA((5,)),
                pltpu.SemaphoreType.DMA((3 + DEPTH, 5)),
                pltpu.SemaphoreType.DMA((BLOCKS + 1, 3 + DEPTH, 5)),
            ],
            compiler_params=pltpu.CompilerParams(collective_id=0, has_side_effects=True, vmem_limit_bytes=56 * 2**20),
        )(frames, w_x, w_h, gate_bias.reshape(1, 256), h_init, c_init)
        return pl.pallas_call(
            write_out,
            out_shape=(jax.ShapeDtypeStruct(frames.shape, BF16), jax.ShapeDtypeStruct(c_init.shape, F32)),
            in_specs=[vmem, vmem],
            out_specs=(hbm, hbm),
            scratch_shapes=[pltpu.SemaphoreType.DMA((STEPS + 1,))],
            compiler_params=pltpu.CompilerParams(vmem_limit_bytes=16 * 2**20),
        )(h_pairs, c_pairs)

    return jax.shard_map(local_run, mesh=mesh, in_specs=(frame_spec, P(), P(), P(), state_spec, state_spec),
                         out_specs=(frame_spec, state_spec), check_vma=False)
```
